8 devices in a mesh: dp: 1 (over z), ep: 8 (over y, x, core).
Axes of the slice: x: 2, y: 2, z: 1, core: 2. Of those that a mesh axis runs over, the one named last changes fastest.
Arguments:
- tokens: bfloat16 [4096, 1280], P(('dp', 'ep'))
- expert_ids: int32 [4096, 6], P(('dp', 'ep'))
- gate_vals: float32 [4096, 6], P(('dp', 'ep'))
- slots: int32 [4096, 6], P(('dp', 'ep'))
- shared_w1: bfloat16 [1280, 1792], replicated
- shared_w3: bfloat16 [1280, 1792], replicated
- shared_w2: bfloat16 [1792, 1280], replicated
- shared_gate: bfloat16 [1280], replicated
- expert_w1: bfloat16 [64, 1280, 896], P('ep')
- expert_w3: bfloat16 [64, 1280, 896], P('ep')
- expert_w2: bfloat16 [64, 896, 1280], P('ep')
Outputs:
- output: bfloat16 [4096, 1280], P(('dp', 'ep'))
All inputs are finite; a program needn't handle non-finite values.
Results may differ from the reference program's by a relative error of at most 0.00517131.
Values are sent between devices in bfloat16 or wider.
A program may use at most 1 GiB of HBM per device.

```python
import jax
import jax.numpy as jnp
from jax import lax

EP_SIZE = 8
TOKENS_DEV = 512
HIDDEN = 1280
EXPERTS = 64
TOP_K = 6
EXPERT_FF = 896
SHARED_FF = 1792
CAPACITY = 96

NUM_TOKENS = EP_SIZE * TOKENS_DEV
BUF_ROWS = EXPERTS * CAPACITY


def draw_routes(route_key):
    score_key, bias_key, hot_key = jax.random.split(route_key, 3)
    scores = jax.random.randint(score_key, (NUM_TOKENS, EXPERTS), 0, 4096)
    expert_bias = jax.random.randint(bias_key, (EXPERTS,), 0, 1024)
    hot_expert = jax.random.randint(hot_key, (), 0, EXPERTS)
    expert_pos = jnp.arange(EXPERTS)
    forced = ((jnp.arange(NUM_TOKENS) % 2) == 0)[:, None] & (expert_pos[None, :] == hot_expert)
    total_score = scores + expert_bias[None, :] + jnp.where(forced, 8192, 0)
    distinct = total_score * EXPERTS + expert_pos[None, :]
    return lax.top_k(distinct, TOP_K)[1].astype(jnp.int32)


def source_slots(src_ids):
    flat_ids = src_ids.reshape(TOKENS_DEV * TOP_K)
    one_hot = (flat_ids[:, None] == jnp.arange(EXPERTS)[None, :]).astype(jnp.int32)
    earlier = jnp.cumsum(one_hot, axis=0) - one_hot
    position = jnp.sum(earlier * one_hot, axis=1)
    return jnp.where(position < CAPACITY, position, -1).reshape(TOKENS_DEV, TOP_K).astype(jnp.int32)


def normal_stack(stack_key, rows, cols):
    def one_matrix(one_key):
        return (jax.random.normal(one_key, (rows, cols), jnp.float32) * rows ** -0.5).astype(jnp.bfloat16)
    return lax.map(one_matrix, jax.random.split(stack_key, EXPERTS))


def setup_inputs(seed: int = 0, part: int = 0) -> dict:
    part_key = jax.random.fold_in(jax.random.key(seed), part)
    tok_key, route_key, gate_key = jax.random.split(part_key, 3)
    weight_keys = jax.random.split(jax.random.key(seed + 1), 7)
    tokens = jax.random.normal(tok_key, (NUM_TOKENS, HIDDEN), jnp.float32).astype(jnp.bfloat16)
    expert_ids = draw_routes(route_key)
    slots = lax.map(source_slots, expert_ids.reshape(EP_SIZE, TOKENS_DEV, TOP_K)).reshape(NUM_TOKENS, TOP_K)
    gate_vals = jax.random.uniform(gate_key, (NUM_TOKENS, TOP_K), jnp.float32, 0.5, 1.5) * TOP_K ** -0.5
    shared_w1 = (jax.random.normal(weight_keys[0], (HIDDEN, SHARED_FF), jnp.float32) * HIDDEN ** -0.5).astype(jnp.bfloat16)
    shared_w3 = (jax.random.normal(weight_keys[1], (HIDDEN, SHARED_FF), jnp.float32) * HIDDEN ** -0.5).astype(jnp.bfloat16)
    shared_w2 = (jax.random.normal(weight_keys[2], (SHARED_FF, HIDDEN), jnp.float32) * SHARED_FF ** -0.5).astype(jnp.bfloat16)
    shared_gate = (jax.random.normal(weight_keys[3], (HIDDEN,), jnp.float32) * 2.0 * HIDDEN ** -0.5).astype(jnp.bfloat16)
    expert_w1 = normal_stack(weight_keys[4], HIDDEN, EXPERT_FF)
    expert_w3 = normal_stack(weight_keys[5], HIDDEN, EXPERT_FF)
    expert_w2 = normal_stack(weight_keys[6], EXPERT_FF, HIDDEN)
    return {'tokens': tokens, 'expert_ids': expert_ids, 'gate_vals': gate_vals, 'slots': slots, 'shared_w1': shared_w1, 'shared_w3': shared_w3, 'shared_w2': shared_w2, 'shared_gate': shared_gate, 'expert_w1': expert_w1, 'expert_w3': expert_w3, 'expert_w2': expert_w2}


def swiglu_rows(rows, w_up, w_in, w_down):
    act_a = jnp.dot(rows, w_up, preferred_element_type=jnp.float32)
    act_b = jnp.dot(rows, w_in, preferred_element_type=jnp.float32)
    hidden_act = (jax.nn.silu(act_a) * act_b).astype(jnp.bfloat16)
    return jnp.dot(hidden_act, w_down, preferred_element_type=jnp.float32)


def reference(tokens, expert_ids, gate_vals, slots, shared_w1, shared_w3, shared_w2, shared_gate, expert_w1, expert_w3, expert_w2):
    src_tokens = tokens.reshape(EP_SIZE, TOKENS_DEV, HIDDEN)
    kept_mask = slots >= 0
    slot_dest = jnp.where(kept_mask, expert_ids * CAPACITY + slots, BUF_ROWS)
    flat_dest = slot_dest.reshape(EP_SIZE, TOKENS_DEV * TOP_K)
    copy_tok = jnp.arange(TOKENS_DEV * TOP_K, dtype=jnp.int32) // TOP_K

    def dispatch_one(operands):
        src_rows, src_dest = operands
        row_owner = jnp.full((BUF_ROWS + 1,), TOKENS_DEV, jnp.int32).at[src_dest].set(copy_tok)
        return jnp.take(src_rows, row_owner[:BUF_ROWS], axis=0, mode='fill', fill_value=0)

    buffers = lax.map(dispatch_one, (src_tokens, flat_dest))
    per_expert = buffers.reshape(EP_SIZE, EXPERTS, CAPACITY, HIDDEN).transpose(1, 0, 2, 3).reshape(EXPERTS, EP_SIZE * CAPACITY, HIDDEN)

    def expert_one(operands):
        rows, w_up, w_in, w_down = operands
        return swiglu_rows(rows, w_up, w_in, w_down).astype(jnp.bfloat16)

    expert_out = lax.map(expert_one, (per_expert, expert_w1, expert_w3, expert_w2))
    returned = expert_out.reshape(EXPERTS, EP_SIZE, CAPACITY, HIDDEN).transpose(1, 0, 2, 3).reshape(EP_SIZE, BUF_ROWS, HIDDEN)
    weights = jnp.where(kept_mask, gate_vals, 0.0).reshape(EP_SIZE, TOKENS_DEV, TOP_K)
    src_dest = slot_dest.reshape(EP_SIZE, TOKENS_DEV, TOP_K)

    def combine_one(operands):
        src_rows, src_out, src_idx, src_weights = operands
        picked = jnp.take(src_out, src_idx, axis=0, mode='fill', fill_value=0)
        routed = jnp.einsum('tk,tkd->td', src_weights, picked.astype(jnp.float32))
        gate_logit = jnp.dot(src_rows, shared_gate, preferred_element_type=jnp.float32)
        shared_out = jax.nn.sigmoid(gate_logit)[:, None] * swiglu_rows(src_rows, shared_w1, shared_w3, shared_w2)
        return (src_rows.astype(jnp.float32) + shared_out + routed).astype(jnp.bfloat16)

    result = lax.map(combine_one, (src_tokens, returned, src_dest, weights))
    return result.reshape(NUM_TOKENS, HIDDEN)
```

```python
import jax
import jax.numpy as jnp
from jax import lax
from jax.sharding import PartitionSpec as P


def solution(mesh):
    num_ep = mesh.shape['ep']
    row_spec = P(('dp', 'ep'), None)
    replicated = P()
    expert_spec = P('ep', None, None)
    perm_part = [(i, i ^ 1) for i in range(num_ep)]
    perm_n1 = [(i, i ^ 2 if i % 2 == 0 else i ^ 4) for i in range(num_ep)]
    perm_n2 = [(i, i ^ 4 if i % 2 == 0 else i ^ 2) for i in range(num_ep)]

    def device_step(tokens, expert_ids, gate_vals, slots, shared_w1, shared_w3, shared_w2, shared_gate, expert_w1, expert_w3, expert_w2):
        tok_count, hidden = tokens.shape
        top_k = expert_ids.shape[1]
        local_experts = expert_w1.shape[0]
        num_experts = local_experts * num_ep
        capacity = 8 * ((2 * tok_count * top_k + 8 * num_experts - 1) // (8 * num_experts))
        rows = local_experts * capacity
        me = lax.axis_index('ep')
        core = me % 2

        def send(v, perm):
            return lax.ppermute(v, 'ep', perm)

        unit_n1 = send(tokens, perm_n1)
        unit_diag = send(unit_n1, perm_n2)
        unit_n2 = send(tokens, perm_n2)
        units = [unit_n1, unit_diag, unit_n2, tokens]
        pairs = [jnp.stack([u, send(u, perm_part)]) for u in units]

        kept = slots >= 0
        dest = jnp.where(kept, expert_ids * capacity + slots, -1)
        meta = jnp.concatenate([dest.astype(jnp.float32).T, jnp.where(kept, gate_vals, 0.0).T], axis=0)
        all_meta = lax.all_gather(meta, 'ep')
        even = core == 0
        n1 = jnp.where(even, me ^ 2, me ^ 4)
        n2 = jnp.where(even, me ^ 4, me ^ 2)
        p1 = jnp.where(even, (me ^ 1) ^ 4, (me ^ 1) ^ 2)
        p2 = jnp.where(even, (me ^ 1) ^ 2, (me ^ 1) ^ 4)
        srcs = [(n1, p1), (me ^ 6, me ^ 7), (n2, p2), (me, me ^ 1)]

        def experts(pair, src):
            m = jnp.stack([all_meta[src[0]], all_meta[src[1]]])
            d = m[:, :top_k].astype(jnp.int32) - me * rows
            g = m[:, top_k:]
            rid = lax.broadcasted_iota(jnp.int32, (2, rows, tok_count), 1)
            hit = [rid == d[:, k][:, None, :] for k in range(top_k)]
            pick = hit[0]
            gt = jnp.where(hit[0], g[:, 0][:, None, :], 0.0)
            for k in range(1, top_k):
                pick = pick | hit[k]
                gt = jnp.where(hit[k], g[:, k][:, None, :], gt)
            x = jnp.einsum('urt,utd->urd', pick.astype(jnp.bfloat16), pair, preferred_element_type=jnp.float32).astype(jnp.bfloat16)
            x = x.reshape(2, local_experts, capacity, hidden)
            a = jnp.einsum('secd,edf->secf', x, expert_w1, preferred_element_type=jnp.float32)
            b = jnp.einsum('secd,edf->secf', x, expert_w3, preferred_element_type=jnp.float32)
            h = (jax.nn.silu(a) * b).astype(jnp.bfloat16)
            r = jnp.einsum('secf,efd->secd', h, expert_w2, preferred_element_type=jnp.float32).astype(jnp.bfloat16)
            r = r.reshape(2, rows, hidden)
            g1 = lax.reduce_precision(gt, 8, 7)
            g2 = lax.reduce_precision(gt - g1, 8, 7)
            g3 = gt - g1 - g2
            out = 0.0
            for gp in (g1, g2, g3):
                out = out + jnp.einsum('urt,urd->utd', gp.astype(jnp.bfloat16), r, preferred_element_type=jnp.float32)
            return out

        gate_logit = jnp.dot(tokens, shared_gate, preferred_element_type=jnp.float32)
        shared_a = jnp.dot(tokens, shared_w1, preferred_element_type=jnp.float32)
        shared_b = jnp.dot(tokens, shared_w3, preferred_element_type=jnp.float32)
        shared_h = (jax.nn.silu(shared_a) * shared_b).astype(jnp.bfloat16)
        shared_out = jnp.dot(shared_h, shared_w2, preferred_element_type=jnp.float32)

        def chip_sum(part):
            return part[0] + send(part[1], perm_part)

        sum_n1 = chip_sum(experts(pairs[0], srcs[0]))
        got_n1 = send(sum_n1, perm_n1)
        sum_diag = chip_sum(experts(pairs[1], srcs[1]))
        got_diag = send(sum_diag, perm_n1)
        sum_n2 = chip_sum(experts(pairs[2], srcs[2])) + got_diag
        got_n2 = send(sum_n2, perm_n2)
        sum_own = chip_sum(experts(pairs[3], srcs[3]))
        total = tokens.astype(jnp.float32) + jax.nn.sigmoid(gate_logit)[:, None] * shared_out + sum_own + got_n1 + got_n2
        return total.astype(jnp.bfloat16)

    return jax.shard_map(device_step, mesh=mesh, in_specs=(row_spec, row_spec, row_spec, row_spec, replicated, replicated, replicated, replicated, expert_spec, expert_spec, expert_spec), out_specs=row_spec, check_vma=False)
```

```python
import functools

import jax
import jax.numpy as jnp
from jax import lax
from jax.experimental import pallas as pl
from jax.experimental.pallas import tpu as pltpu
from jax.sharding import PartitionSpec as P

SLOTS = 3
CHUNK = 128
f32, bf16 = jnp.float32, jnp.bfloat16


def dot(a, b):
    return jnp.dot(a, b, preferred_element_type=f32)


def moe_kernel(num_ep, local, cap, top_k, meta_ref, tok_ref, gate_ref, sw1, sw3, sw2, ew1, ew3, ew2, out_ref,
               meta_all, tb, r_mine, r_out, r_in, w1s, w3s, w2s, acc, s1, sd, got1, gotd, got2, h_ref, xs, gm,
               w_sem, m_send, m_recv, t_send, t_recv, r_send, r_recv, s_send, s_recv):
    tok_count, hidden = tok_ref.shape
    ff = w1s.shape[2]
    rows = local * cap
    chunks = tok_count // CHUNK
    me = lax.axis_index('ep')
    core, xx, yy = me % 2, (me // 2) % 2, me // 4
    step_x, step_y = 2 - 4 * xx, 4 - 8 * yy
    part = me + 1 - 2 * core
    off1 = (1 - core) * step_x + core * step_y
    off2 = core * step_x + (1 - core) * step_y
    n1, n2, diag = me + off1, me + off2, me + step_x + step_y
    pn1, pn2, pdiag = part + off2, part + off1, part + step_x + step_y

    def remote(src, dst, ss, rs, dev):
        return pltpu.make_async_remote_copy(src_ref=src, dst_ref=dst, send_sem=ss, recv_sem=rs,
                                            device_id={'ep': dev}, device_id_type=pl.DeviceIdType.MESH)

    def weight_copies(src1, src3, src2, slot):
        return [pltpu.make_async_copy(src1, w1s.at[slot], w_sem.at[slot, 0]),
                pltpu.make_async_copy(src3, w3s.at[slot], w_sem.at[slot, 1]),
                pltpu.make_async_copy(src2, w2s.at[slot], w_sem.at[slot, 2])]

    def start_expert(e, slot):
        for c in weight_copies(ew1.at[e], ew3.at[e], ew2.at[e], slot):
            c.start()

    def wait_weights(slot):
        for c in weight_copies(ew1.at[0], ew3.at[0], ew2.at[0], slot):
            c.wait()

    for s in range(2):
        cols = pl.ds(s * ff, ff)
        for c in weight_copies(sw1.at[:, cols], sw3.at[:, cols], sw2.at[cols, :], s):
            c.start()
    start_expert(0, 2)

    barrier = pltpu.get_barrier_semaphore()
    for k in range(1, num_ep):
        pl.semaphore_signal(barrier, inc=1, device_id={'ep': (me + k) % num_ep}, device_id_type=pl.DeviceIdType.MESH)
    pl.semaphore_wait(barrier, num_ep - 1)

    meta_copies = [remote(meta_ref, meta_all.at[me], m_send.at[k - 1], m_recv.at[k - 1], (me + k) % num_ep) for k in range(1, num_ep)]
    for c in meta_copies:
        c.start()
    t_own = remote(tok_ref, tb.at[0], t_send.at[0], t_recv.at[0], part)
    t_n1 = remote(tok_ref, tb.at[1], t_send.at[1], t_recv.at[1], n1)
    t_n1p = remote(tb.at[1], tb.at[2], t_send.at[2], t_recv.at[2], part)
    t_d = remote(tb.at[1], tb.at[3], t_send.at[3], t_recv.at[3], n2)
    t_dp = remote(tb.at[3], tb.at[4], t_send.at[4], t_recv.at[4], part)
    t_n2 = remote(tok_ref, tb.at[5], t_send.at[5], t_recv.at[5], n2)
    t_n2p = remote(tb.at[5], tb.at[6], t_send.at[6], t_recv.at[6], part)
    t_n1.start()
    t_own.start()
    meta_all[me] = meta_ref[...]

    def swiglu_up(x, slot, put):
        full = ff // 256
        for c in range(full):
            cols = slice(c * 256, c * 256 + 256)
            a = dot(x, w1s[slot, :, cols])
            b = dot(x, w3s[slot, :, cols])
            put(cols, (jax.nn.silu(a) * b).astype(bf16))
        cols = slice(full * 256, ff)
        rest = ff - full * 256
        ab = dot(x, jnp.concatenate([w1s[slot, :, cols], w3s[slot, :, cols]], axis=1))
        put(cols, (jax.nn.silu(ab[:, :rest]) * ab[:, rest:]).astype(bf16))

    mrows = 256

    def shared_half(s):
        wait_weights(s)

        def block(i, _):
            rs = pl.ds(pl.multiple_of(i * mrows, mrows), mrows)

            def put(cols, v):
                h_ref[rs, cols] = v
            swiglu_up(tok_ref[rs, :], s, put)
            if s == 1:
                logit = jnp.sum(tok_ref[rs, :].astype(f32) * gate_ref[...].astype(f32), axis=1, keepdims=True)
                sig = jax.nn.sigmoid(logit)
            for n in range(hidden // 256):
                cols = slice(n * 256, n * 256 + 256)
                v = dot(h_ref[rs, :], w2s[s, :, cols])
                if s == 0:
                    acc[rs, cols] = v
                else:
                    acc[rs, cols] = tok_ref[rs, cols].astype(f32) + sig * (acc[rs, cols] + v)
            return 0
        lax.fori_loop(0, tok_count // mrows, block, 0)
        start_expert(s + 1, s)

    shared_half(0)
    shared_half(1)
    for c in meta_copies:
        c.wait()

    t_n1.wait_recv()
    t_d.start()
    t_n1p.start()
    t_n2.start()
    t_n1p.wait_recv()

    lane_row = lax.broadcasted_iota(jnp.int32, (cap, tok_count), 0).astype(f32)
    lane_col = lax.broadcasted_iota(jnp.int32, (CHUNK, 128), 1).astype(f32)

    def expert_loop(p, mine, other, src, psrc):
        par = p % 2

        def body(e, _):
            slot = (p * local + 2 + e) % SLOTS
            base = ((me * local + e) * cap).astype(f32)
            for u, (unit, who) in enumerate(((mine, src), (other, psrc))):
                d = meta_all[who, 0:8, :] - base
                hit = d[0:1, :] == lane_row
                for k in range(1, top_k):
                    hit = hit | (d[k:k + 1, :] == lane_row)
                pick = jnp.where(hit, 1.0, 0.0).astype(bf16)
                for n in range(hidden // 256):
                    cols = slice(n * 256, n * 256 + 256)
                    xs[u * cap:(u + 1) * cap, cols] = dot(pick, unit[:, cols]).astype(bf16)
            wait_weights(slot)

            def put(cols, v):
                h_ref[0:2 * cap, cols] = v
            swiglu_up(xs[...], slot, put)
            rs = pl.ds(pl.multiple_of(e * cap, cap), cap)
            for n in range(hidden // 256):
                cols = slice(n * 256, n * 256 + 256)
                v = dot(h_ref[0:2 * cap, :], w2s[slot, :, cols]).astype(bf16)
                r_mine[rs, cols] = v[:cap]
                r_out[rs, cols] = v[cap:]
            remote(r_out.at[rs], r_in.at[par, rs], r_send, r_recv.at[par], part).start()
            if p < 3:
                start_expert((e + SLOTS) % local, slot)
            else:
                @pl.when(e + SLOTS < local)
                def _():
                    start_expert(e + SLOTS, slot)
            return 0
        lax.fori_loop(0, local, body, 0)

    def combine(p, src, store, send):
        par = p % 2
        whole = remote(r_out, r_in.at[par], r_send, r_recv.at[par], part)
        whole.wait()
        nr = rows // 128

        def block(i, _):
            rs = pl.ds(pl.multiple_of(i * CHUNK, CHUNK), CHUNK)
            m = jnp.transpose(meta_all[src, :, rs])
            for half, owner in enumerate((me, part)):
                base = (owner * rows).astype(f32)
                for c in range(nr):
                    rid = lane_col + (base + c * 128.0)
                    g = jnp.where(m[:, 0:1] == rid, m[:, 8:9], 0.0)
                    for k in range(1, top_k):
                        g = jnp.where(m[:, k:k + 1] == rid, m[:, 8 + k:9 + k], g)
                    g1 = g.astype(bf16)
                    rem = g - g1.astype(f32)
                    g2 = rem.astype(bf16)
                    g3 = (rem - g2.astype(f32)).astype(bf16)
                    lanes = slice(half * rows + c * 128, half * rows + c * 128 + 128)
                    gm[0, :, lanes] = g1
                    gm[1, :, lanes] = g2
                    gm[2, :, lanes] = g3
            for n in range(hidden // 256):
                cols = slice(n * 256, n * 256 + 256)
                v = None
                for q in range(3):
                    t = dot(gm[q, :, 0:rows], r_mine[:, cols]) + dot(gm[q, :, rows:], r_in[par, :, cols])
                    v = t if v is None else v + t
                store(rs, cols, v + v)
            send(i, rs)
            return 0
        lax.fori_loop(0, chunks, block, 0)

    def chunk_rows(c):
        return pl.ds(c * CHUNK, CHUNK)

    def put_s1(rs, cols, v):
        s1[rs, cols] = v

    def put_sd(rs, cols, v):
        sd[rs, cols] = v

    def put_acc(rs, cols, v):
        acc[rs, cols] = acc[rs, cols] + v

    def s_copy(which, src, dst, c, rs, dev):
        return remote(src.at[rs], dst.at[rs], s_send.at[which, c], s_recv.at[which, c], dev)

    def no_send(i, rs):
        pass

    expert_loop(0, tb.at[1], tb.at[2], n1, pn1)
    t_d.wait_recv()
    t_dp.start()
    combine(0, n1, put_s1, lambda i, rs: s_copy(0, s1, got1, i, rs, n1).start())
    t_dp.wait_recv()

    expert_loop(1, tb.at[3], tb.at[4], diag, pdiag)
    t_n2.wait_recv()
    t_n2p.start()
    combine(1, diag, put_sd, lambda i, rs: s_copy(1, sd, gotd, i, rs, n1).start())
    t_n2p.wait_recv()

    expert_loop(2, tb.at[5], tb.at[6], n2, pn2)
    for c in range(chunks):
        s_copy(0, s1, got1, c, chunk_rows(c), n1).wait_send()
    combine(2, n2, put_s1, no_send)
    t_own.wait_recv()

    expert_loop(3, tok_ref, tb.at[0], me, part)
    combine(3, me, put_acc, no_send)

    for c in range(chunks):
        rs = chunk_rows(c)
        s_copy(1, sd, gotd, c, rs, n1).wait_recv()
        s1[rs, :] = s1[rs, :] + gotd[rs, :]
        s_copy(2, s1, got2, c, rs, n2).start()
    for c in range(chunks):
        rs = chunk_rows(c)
        s_copy(0, s1, got1, c, rs, n1).wait_recv()
        s_copy(2, s1, got2, c, rs, n2).wait_recv()
        out_ref[rs, :] = (acc[rs, :] + got1[rs, :] + got2[rs, :]).astype(bf16)
    for c in range(chunks):
        rs = chunk_rows(c)
        s_copy(1, sd, gotd, c, rs, n1).wait_send()
        s_copy(2, s1, got2, c, rs, n2).wait_send()
    for t in (t_own, t_n1, t_n1p, t_d, t_dp, t_n2, t_n2p):
        t.wait_send()


def solution(mesh):
    num_ep = mesh.shape['ep']
    row_spec = P(('dp', 'ep'), None)
    replicated = P()
    expert_spec = P('ep', None, None)

    def device_step(tokens, expert_ids, gate_vals, slots, shared_w1, shared_w3, shared_w2, shared_gate, expert_w1, expert_w3, expert_w2):
        tok_count, hidden = tokens.shape
        top_k = expert_ids.shape[1]
        local, _, ff = expert_w1.shape
        num_experts = local * num_ep
        cap = 8 * ((2 * tok_count * top_k + 8 * num_experts - 1) // (8 * num_experts))
        rows = local * cap
        chunks = tok_count // CHUNK
        kept = slots >= 0
        dest = jnp.where(kept, expert_ids * cap + slots, -1).astype(f32)
        pad = ((0, 8 - top_k), (0, 0))
        meta = jnp.concatenate([jnp.pad(dest.T, pad, constant_values=-1.0), jnp.pad(jnp.where(kept, 0.5 * gate_vals, 0.0).T, pad)], axis=0)
        vm = pl.BlockSpec(memory_space=pltpu.VMEM)
        hbm = pl.BlockSpec(memory_space=pltpu.HBM)
        dma = pltpu.SemaphoreType.DMA
        return pl.pallas_call(
            functools.partial(moe_kernel, num_ep, local, cap, top_k),
            out_shape=jax.ShapeDtypeStruct((tok_count, hidden), bf16),
            in_specs=[vm, vm, vm] + [hbm] * 6,
            out_specs=vm,
            scratch_shapes=[
                pltpu.VMEM((num_ep, 16, tok_count), f32),
                pltpu.VMEM((7, tok_count, hidden), bf16),
                pltpu.VMEM((rows, hidden), bf16),
                pltpu.VMEM((rows, hidden), bf16),
                pltpu.VMEM((2, rows, hidden), bf16),
                pltpu.VMEM((SLOTS, hidden, ff), bf16),
                pltpu.VMEM((SLOTS, hidden, ff), bf16),
                pltpu.VMEM((SLOTS, ff, hidden), bf16),
            ] + [pltpu.VMEM((tok_count, hidden), f32)] * 6 + [
                pltpu.VMEM((tok_count, ff), bf16),
                pltpu.VMEM((2 * cap, hidden), bf16),
                pltpu.VMEM((3, CHUNK, 2 * rows), bf16),
                dma((SLOTS, 3)), dma((num_ep - 1,)), dma((num_ep - 1,)), dma((7,)), dma((7,)),
                dma, dma((2,)), dma((3, chunks)), dma((3, chunks)),
            ],
            compiler_params=pltpu.CompilerParams(collective_id=0, has_side_effects=True, vmem_limit_bytes=67043328),
        )(meta, tokens, shared_gate.reshape(1, hidden), shared_w1, shared_w3, shared_w2, expert_w1, expert_w3, expert_w2)

    return jax.shard_map(device_step, mesh=mesh, in_specs=(row_spec, row_spec, row_spec, row_spec, replicated, replicated, replicated, replicated, expert_spec, expert_spec, expert_spec), out_specs=row_spec, check_vma=False)
```

```python
import functools

import jax
import jax.numpy as jnp
from jax import lax
from jax.experimental import pallas as pl
from jax.experimental.pallas import tpu as pltpu
from jax.sharding import PartitionSpec as P

SLOTS = 3
CHUNK = 128
f32, bf16 = jnp.float32, jnp.bfloat16


def dot(a, b):
    return jnp.dot(a, b, preferred_element_type=f32)


def moe_kernel(num_ep, local, cap, top_k, ids_ref, slot_ref, gval_ref, tok_ref, gate_ref, sw1, sw3, sw2, ew1, ew3, ew2, out_ref,
               tb, mb, r_mine, r_out, r_in, w1s, w3s, w2s, s1, sd, got1, gotd, got2, h_ref, xs, gma, gmb,
               w_sem, t_send, t_recv, m_send, m_recv, r_send, r_recv, s_send, s_recv):
    tok_count, hidden = tok_ref.shape
    ff = w1s.shape[2]
    rows = local * cap
    chunks = tok_count // CHUNK
    me = lax.axis_index('ep')
    core, xx, yy = me % 2, (me // 2) % 2, me // 4
    step_x, step_y = 2 - 4 * xx, 4 - 8 * yy
    part = me + 1 - 2 * core
    n1 = me + (1 - core) * step_x + core * step_y
    n2 = me + core * step_x + (1 - core) * step_y

    def remote(src, dst, ss, rs, dev):
        return pltpu.make_async_remote_copy(src_ref=src, dst_ref=dst, send_sem=ss, recv_sem=rs,
                                            device_id={'ep': dev}, device_id_type=pl.DeviceIdType.MESH)

    def weight_copies(src1, src3, src2, slot):
        return [pltpu.make_async_copy(src1, w1s.at[slot], w_sem.at[slot, 0]),
                pltpu.make_async_copy(src3, w3s.at[slot], w_sem.at[slot, 1]),
                pltpu.make_async_copy(src2, w2s.at[slot], w_sem.at[slot, 2])]

    def start_expert(e, slot):
        for c in weight_copies(ew1.at[e], ew3.at[e], ew2.at[e], slot):
            c.start()

    def start_shared(s, slot):
        cols = pl.ds(s * ff, ff)
        for c in weight_copies(sw1.at[:, cols], sw3.at[:, cols], sw2.at[cols, :], slot):
            c.start()

    def wait_weights(slot):
        for c in weight_copies(ew1.at[0], ew3.at[0], ew2.at[0], slot):
            c.wait()

    for e in range(SLOTS):
        start_expert(e, e)

    kept = slot_ref[...] >= 0
    mb[7, 0:top_k, :] = jnp.where(kept, ids_ref[...] * cap + slot_ref[...], -1).astype(f32)
    mb[7, top_k:8, :] = jnp.full((8 - top_k, tok_count), -1.0, f32)
    mb[7, 8:8 + top_k, :] = jnp.where(kept, 0.5 * gval_ref[...], 0.0)
    mb[7, 8 + top_k:16, :] = jnp.zeros((8 - top_k, tok_count), f32)

    barrier = pltpu.get_barrier_semaphore()
    for k in range(1, num_ep):
        pl.semaphore_signal(barrier, inc=1, device_id={'ep': (me + k) % num_ep}, device_id_type=pl.DeviceIdType.MESH)
    pl.semaphore_wait(barrier, num_ep - 1)

    class Hop:
        def __init__(self, src, dst, dev):
            self.copies = (remote(mb.at[src], mb.at[dst], m_send.at[dst], m_recv.at[dst], dev),
                           remote(tok_ref if src == 7 else tb.at[src], tb.at[dst], t_send.at[dst], t_recv.at[dst], dev))

        def start(self):
            for c in self.copies:
                c.start()

        def wait_recv(self):
            for c in self.copies:
                c.wait_recv()

        def wait_send(self):
            for c in self.copies:
                c.wait_send()

    t_own, t_n1, t_n1p, t_d, t_dp, t_n2, t_n2p = (
        Hop(7, 0, part), Hop(7, 1, n1), Hop(1, 2, part), Hop(1, 3, n2), Hop(3, 4, part), Hop(7, 5, n2), Hop(5, 6, part))
    t_n1.start()
    t_own.start()

    def swiglu_up(x, slot, put):
        full = ff // 256
        for c in range(full):
            cols = slice(c * 256, c * 256 + 256)
            a = dot(x, w1s[slot, :, cols])
            b = dot(x, w3s[slot, :, cols])
            put(cols, (jax.nn.silu(a) * b).astype(bf16))
        cols = slice(full * 256, ff)
        rest = ff - full * 256
        ab = dot(x, jnp.concatenate([w1s[slot, :, cols], w3s[slot, :, cols]], axis=1))
        put(cols, (jax.nn.silu(ab[:, :rest]) * ab[:, rest:]).astype(bf16))

    lane_row = lax.broadcasted_iota(jnp.int32, (cap, tok_count), 0).astype(f32)
    lane_col = lax.broadcasted_iota(jnp.int32, (CHUNK, 128), 1).astype(f32)

    def whole_rows(par):
        return remote(r_out, r_in.at[par], r_send, r_recv.at[par], part)

    def expert_loop(order, par, keep, mine, other, mi, oi, late=None):
        def dispatch(e):
            base = ((me * local + e) * cap).astype(f32)
            for u, (unit, who) in enumerate(((mine, mi), (other, oi))):
                d = mb[who, 0:8, :] - base
                hit = d[0:1, :] == lane_row
                for k in range(1, top_k):
                    hit = hit | (d[k:k + 1, :] == lane_row)
                pick = jnp.where(hit, 1.0, 0.0).astype(bf16)
                for n in range(hidden // 256):
                    cols = slice(n * 256, n * 256 + 256)
                    xs[u * cap:(u + 1) * cap, cols] = dot(pick, unit[:, cols]).astype(bf16)

        dispatch(jnp.int32(0))

        def body(e, _):
            if late is not None:
                pl.when(e == local - 1)(late)
            slot = (order * local + e) % SLOTS
            wait_weights(slot)

            def put(cols, v):
                h_ref[0:2 * cap, cols] = v
            swiglu_up(xs[...], slot, put)
            dispatch(e + 1)
            rs = pl.ds(pl.multiple_of(e * cap, cap), cap)
            for n in range(hidden // 256):
                cols = slice(n * 256, n * 256 + 256)
                v = dot(h_ref[0:2 * cap, :], w2s[slot, :, cols]).astype(bf16)
                r_mine[keep, rs, cols] = v[:cap]
                r_out[rs, cols] = v[cap:]
            remote(r_out.at[rs], r_in.at[par, rs], r_send, r_recv.at[par], part).start()
            if order < 3:
                start_expert((e + SLOTS) % local, slot)
            else:
                @pl.when(e + SLOTS < local)
                def _():
                    start_expert(e + SLOTS, slot)
                for s in range(2):
                    @pl.when(e + SLOTS == local + s)
                    def _():
                        start_shared(s, slot)
            return 0
        lax.fori_loop(0, local, body, 0)

    def combine(par, keep, mi, ready, store, send, wait_rows):
        nr = rows // 128

        def build(i, gm):
            rs = pl.ds(pl.multiple_of(i * CHUNK, CHUNK), CHUNK)
            m = jnp.transpose(mb[mi, :, rs])
            for half, owner in enumerate((me, part)):
                base = (owner * rows).astype(f32)
                for c in range(nr):
                    rid = lane_col + (base + c * 128.0)
                    g = jnp.where(m[:, 0:1] == rid, m[:, 8:9], 0.0)
                    for k in range(1, top_k):
                        g = jnp.where(m[:, k:k + 1] == rid, m[:, 8 + k:9 + k], g)
                    g1 = g.astype(bf16)
                    rem = g - g1.astype(f32)
                    g2 = rem.astype(bf16)
                    g3 = (rem - g2.astype(f32)).astype(bf16)
                    lanes = slice(half * rows + c * 128, half * rows + c * 128 + 128)
                    gm[0, :, lanes] = g1
                    gm[1, :, lanes] = g2
                    gm[2, :, lanes] = g3

        def products(i, gm):
            rs = pl.ds(pl.multiple_of(i * CHUNK, CHUNK), CHUNK)
            for n in range(hidden // 256):
                cols = slice(n * 256, n * 256 + 256)
                v = None
                for q in range(3):
                    t = dot(gm[q, :, 0:rows], r_mine[keep, :, cols]) + dot(gm[q, :, rows:], r_in[par, :, cols])
                    v = t if v is None else v + t
                store(rs, cols, v + v)

        build(jnp.int32(0), gma)
        wait_rows()

        def pair(j, _):
            for t, (now, later) in enumerate(((gma, gmb), (gmb, gma))):
                i = 2 * j + t
                rs = pl.ds(pl.multiple_of(i * CHUNK, CHUNK), CHUNK)
                ready(i, rs)
                build((i + 1) % chunks, later)
                products(i, now)
                send(i, rs)
            return 0
        lax.fori_loop(0, chunks // 2, pair, 0)

    def chunk_rows(c):
        return pl.ds(c * CHUNK, CHUNK)

    def s_copy(which, c, rs):
        src, dst, dev = ((s1, got1, n1), (sd, gotd, n1), (s1, got2, n2))[which]
        return remote(src.at[rs], dst.at[rs], s_send.at[which, c], s_recv.at[which, c], dev)

    def put_s1(rs, cols, v):
        s1[rs, cols] = v

    def put_sd(rs, cols, v):
        sd[rs, cols] = v

    def put_s2(rs, cols, v):
        s1[rs, cols] = v + gotd[rs, cols]

    def nothing(i, rs):
        pass

    def first_tokens():
        t_n1.wait_recv()
        t_d.start()
        t_n1p.start()
        t_n2.start()

    t_own.wait_recv()
    expert_loop(0, 2, 1, tok_ref, tb.at[0], 7, 0, late=first_tokens)
    t_n1p.wait_recv()
    whole_rows(2).wait_send()

    expert_loop(1, 0, 0, tb.at[1], tb.at[2], 1, 2)
    t_d.wait_recv()
    t_dp.start()
    combine(0, 0, 1, nothing, put_s1, lambda i, rs: s_copy(0, i, rs).start(), lambda: whole_rows(0).wait())
    t_dp.wait_recv()

    expert_loop(2, 1, 0, tb.at[3], tb.at[4], 3, 4)
    t_n2.wait_recv()
    t_n2p.start()
    combine(1, 0, 3, nothing, put_sd, lambda i, rs: s_copy(1, i, rs).start(), lambda: whole_rows(1).wait())
    t_n2p.wait_recv()

    expert_loop(3, 0, 0, tb.at[5], tb.at[6], 5, 6)
    for c in range(chunks):
        s_copy(0, c, chunk_rows(c)).wait_send()
    combine(0, 0, 5, lambda i, rs: s_copy(1, i, rs).wait_recv(), put_s2, lambda i, rs: s_copy(2, i, rs).start(),
            lambda: whole_rows(0).wait())

    for c in range(chunks):
        s_copy(1, c, chunk_rows(c)).wait_send()
    combine(2, 1, 7, nothing, put_sd, nothing, lambda: whole_rows(2).wait_recv())

    mrows = 256
    for s in range(2):
        slot = (4 * local + s) % SLOTS
        wait_weights(slot)

        def block(i, _):
            rs = pl.ds(pl.multiple_of(i * mrows, mrows), mrows)

            def put(cols, v):
                h_ref[:, cols] = v
            swiglu_up(tok_ref[rs, :], slot, put)
            logit = jnp.sum(tok_ref[rs, :].astype(f32) * gate_ref[...].astype(f32).reshape(1, hidden), axis=1, keepdims=True)
            sig = jax.nn.sigmoid(logit)
            for n in range(hidden // 256):
                cols = slice(n * 256, n * 256 + 256)
                v = sd[rs, cols] + sig * dot(h_ref[...], w2s[slot, :, cols])
                if s == 1:
                    v = v + tok_ref[rs, cols].astype(f32)
                sd[rs, cols] = v
            return 0
        lax.fori_loop(0, tok_count // mrows, block, 0)

    for c in range(chunks):
        rs = chunk_rows(c)
        s_copy(0, c, rs).wait_recv()
        s_copy(2, c, rs).wait_recv()
        out_ref[rs, :] = (sd[rs, :] + got1[rs, :] + got2[rs, :]).astype(bf16)
    for c in range(chunks):
        s_copy(2, c, chunk_rows(c)).wait_send()
    for t in (t_own, t_n1, t_n1p, t_d, t_dp, t_n2, t_n2p):
        t.wait_send()


def solution(mesh):
    num_ep = mesh.shape['ep']
    row_spec = P(('dp', 'ep'), None)
    replicated = P()
    expert_spec = P('ep', None, None)

    def device_step(tokens, expert_ids, gate_vals, slots, shared_w1, shared_w3, shared_w2, shared_gate, expert_w1, expert_w3, expert_w2):
        tok_count, hidden = tokens.shape
        top_k = expert_ids.shape[1]
        local, _, ff = expert_w1.shape
        num_experts = local * num_ep
        cap = 8 * ((2 * tok_count * top_k + 8 * num_experts - 1) // (8 * num_experts))
        rows = local * cap
        chunks = tok_count // CHUNK
        vm = pl.BlockSpec(memory_space=pltpu.VMEM)
        hbm = pl.BlockSpec(memory_space=pltpu.HBM)
        dma = pltpu.SemaphoreType.DMA
        return pl.pallas_call(
            functools.partial(moe_kernel, num_ep, local, cap, top_k),
            out_shape=jax.ShapeDtypeStruct((tok_count, hidden), bf16),
            in_specs=[vm] * 5 + [hbm] * 6,
            out_specs=vm,
            scratch_shapes=[
                pltpu.VMEM((7, tok_count, hidden), bf16),
                pltpu.VMEM((8, 16, tok_count), f32),
                pltpu.VMEM((2, rows, hidden), bf16),
                pltpu.VMEM((rows, hidden), bf16),
                pltpu.VMEM((3, rows, hidden), bf16),
                pltpu.VMEM((SLOTS, hidden, ff), bf16),
                pltpu.VMEM((SLOTS, hidden, ff), bf16),
                pltpu.VMEM((SLOTS, ff, hidden), bf16),
            ] + [pltpu.VMEM((tok_count, hidden), f32)] * 5 + [
                pltpu.VMEM((256, ff), bf16),
                pltpu.VMEM((2 * cap, hidden), bf16),
                pltpu.VMEM((3, CHUNK, 2 * rows), bf16),
                pltpu.VMEM((3, CHUNK, 2 * rows), bf16),
                dma((SLOTS, 3)), dma((7,)), dma((7,)), dma((7,)), dma((7,)),
                dma, dma((3,)), dma((3, chunks)), dma((3, chunks)),
            ],
            compiler_params=pltpu.CompilerParams(collective_id=0, has_side_effects=True, vmem_limit_bytes=67043328),
        )(expert_ids.T, slots.T, gate_vals.T, tokens, shared_gate, shared_w1, shared_w3, shared_w2, expert_w1, expert_w3, expert_w2)

    return jax.shard_map(device_step, mesh=mesh, in_specs=(row_spec, row_spec, row_spec, row_spec, replicated, replicated, replicated, replicated, expert_spec, expert_spec, expert_spec), out_specs=row_spec, check_vma=False)
```

```python
import functools

import jax
import jax.numpy as jnp
from jax import lax
from jax.experimental import pallas as pl
from jax.experimental.pallas import tpu as pltpu
from jax.sharding import PartitionSpec as P

SLOTS = 3
CHUNK = 128
HEAD = 256
f32, bf16 = jnp.float32, jnp.bfloat16


def dot(a, b):
    return jnp.dot(a, b, preferred_element_type=f32)


def moe_kernel(num_ep, local, cap, top_k, ids_hbm, slot_hbm, gval_hbm, tok_hbm, gate_ref, sw1, sw3, sw2, ew1, ew3, ew2, out_hbm,
               out_ref, tok_ref, ids_ref, slot_ref, gval_ref, tb, mb, r_mine, r_out, r_in, w1s, w3s, w2s, s1, sd, got1, gotd, got2, h_ref, xs, gma, gmb,
               i_sem, o_sem, w_sem, t_send, t_recv, m_send, m_recv, r_send, r_recv, s_send, s_recv):
    tok_count, hidden = tok_ref.shape
    ff = w1s.shape[2]
    rows = local * cap
    chunks = tok_count // CHUNK
    me = lax.axis_index('ep')
    core, xx, yy = me % 2, (me // 2) % 2, me // 4
    step_x, step_y = 2 - 4 * xx, 4 - 8 * yy
    part = me + 1 - 2 * core
    n1 = me + (1 - core) * step_x + core * step_y
    n2 = me + core * step_x + (1 - core) * step_y

    def remote(src, dst, ss, rs, dev):
        return pltpu.make_async_remote_copy(src_ref=src, dst_ref=dst, send_sem=ss, recv_sem=rs,
                                            device_id={'ep': dev}, device_id_type=pl.DeviceIdType.MESH)

    def weight_copies(src1, src3, src2, slot):
        return [pltpu.make_async_copy(src1, w1s.at[slot], w_sem.at[slot, 0]),
                pltpu.make_async_copy(src3, w3s.at[slot], w_sem.at[slot, 1]),
                pltpu.make_async_copy(src2, w2s.at[slot], w_sem.at[slot, 2])]

    def start_expert(e, slot):
        for c in weight_copies(ew1.at[e], ew3.at[e], ew2.at[e], slot):
            c.start()

    def start_shared(s, slot):
        cols = pl.ds(s * ff, ff)
        for c in weight_copies(sw1.at[:, cols], sw3.at[:, cols], sw2.at[cols, :], slot):
            c.start()

    def wait_weights(slot):
        for c in weight_copies(ew1.at[0], ew3.at[0], ew2.at[0], slot):
            c.wait()

    barrier = pltpu.get_barrier_semaphore()
    for dev in (n1, n2, part):
        pl.semaphore_signal(barrier, inc=1, device_id={'ep': dev}, device_id_type=pl.DeviceIdType.MESH)
    loads = [pltpu.make_async_copy(src, dst, i_sem.at[k]) for k, (src, dst) in enumerate((
        (ids_hbm, ids_ref), (slot_hbm, slot_ref), (gval_hbm, gval_ref), (tok_hbm, tok_ref)))]
    for c in loads:
        c.start()
    for c in loads:
        c.wait()
    for e in range(SLOTS):
        start_expert(e, e)

    kept = slot_ref[...] >= 0
    mb[7, 0:top_k, :] = jnp.where(kept, ids_ref[...] * cap + slot_ref[...], -1).astype(f32)
    mb[7, top_k:8, :] = jnp.full((8 - top_k, tok_count), -1.0, f32)
    mb[7, 8:8 + top_k, :] = jnp.where(kept, 0.5 * gval_ref[...], 0.0)
    mb[7, 8 + top_k:16, :] = jnp.zeros((8 - top_k, tok_count), f32)

    pl.semaphore_wait(barrier, 3)

    class Hop:
        def __init__(self, src, dst, dev):
            self.copies = (remote(mb.at[src], mb.at[dst], m_send.at[dst], m_recv.at[dst], dev),
                           remote(tok_ref if src == 7 else tb.at[src], tb.at[dst], t_send.at[dst], t_recv.at[dst], dev))

        def start(self):
            for c in self.copies:
                c.start()

        def wait_recv(self):
            for c in self.copies:
                c.wait_recv()

        def wait_send(self):
            for c in self.copies:
                c.wait_send()

    t_own, t_n1, t_n1p, t_d, t_dp, t_n2, t_n2p = (
        Hop(7, 0, part), Hop(7, 1, n1), Hop(1, 2, part), Hop(1, 3, n2), Hop(3, 4, part), Hop(7, 5, n2), Hop(5, 6, part))
    head, tail = pl.ds(0, HEAD), pl.ds(HEAD, tok_count - HEAD)
    t_head = remote(tok_ref.at[head], tb.at[5, head], t_send.at[7], t_recv.at[7], n2)
    t_n2.copies = (t_n2.copies[0], remote(tok_ref.at[tail], tb.at[5, tail], t_send.at[5], t_recv.at[5], n2))
    t_n1.start()
    t_own.start()

    def swiglu_up(x, slot, put):
        full = ff // 256
        for c in range(full):
            cols = slice(c * 256, c * 256 + 256)
            a = dot(x, w1s[slot, :, cols])
            b = dot(x, w3s[slot, :, cols])
            put(cols, (jax.nn.silu(a) * b).astype(bf16))
        cols = slice(full * 256, ff)
        rest = ff - full * 256
        ab = dot(x, jnp.concatenate([w1s[slot, :, cols], w3s[slot, :, cols]], axis=1))
        put(cols, (jax.nn.silu(ab[:, :rest]) * ab[:, rest:]).astype(bf16))

    lane_row = lax.broadcasted_iota(jnp.int32, (cap, tok_count), 0).astype(f32)
    lane_col = lax.broadcasted_iota(jnp.int32, (CHUNK, 128), 1).astype(f32)

    def whole_rows(par):
        return remote(r_out, r_in.at[par], r_send, r_recv.at[par], part)

    def expert_loop(order, par, keep, mine, other, mi, oi, late=()):
        def dispatch(e):
            base = ((me * local + e) * cap).astype(f32)
            for u, (unit, who) in enumerate(((mine, mi), (other, oi))):
                d = mb[who, 0:8, :] - base
                hit = d[0:1, :] == lane_row
                for k in range(1, top_k):
                    hit = hit | (d[k:k + 1, :] == lane_row)
                pick = jnp.where(hit, 1.0, 0.0).astype(bf16)
                for n in range(hidden // 256):
                    cols = slice(n * 256, n * 256 + 256)
                    xs[u * cap:(u + 1) * cap, cols] = dot(pick, unit[:, cols]).astype(bf16)

        dispatch(jnp.int32(0))

        def body(e, _):
            for at, what in late:
                pl.when(e == at)(what)
            slot = (order * local + e) % SLOTS
            wait_weights(slot)

            def put(cols, v):
                h_ref[0:2 * cap, cols] = v
            swiglu_up(xs[...], slot, put)
            dispatch(e + 1)
            rs = pl.ds(pl.multiple_of(e * cap, cap), cap)
            for n in range(hidden // 256):
                cols = slice(n * 256, n * 256 + 256)
                v = dot(h_ref[0:2 * cap, :], w2s[slot, :, cols]).astype(bf16)
                r_mine[keep, rs, cols] = v[:cap]
                r_out[rs, cols] = v[cap:]
            remote(r_out.at[rs], r_in.at[par, rs], r_send, r_recv.at[par], part).start()
            if order < 3:
                start_expert((e + SLOTS) % local, slot)
            else:
                @pl.when(e + SLOTS < local)
                def _():
                    start_expert(e + SLOTS, slot)
                for s in range(2):
                    @pl.when(e + SLOTS == local + s)
                    def _():
                        start_shared(s, slot)
            return 0
        lax.fori_loop(0, local, body, 0)

    def combine(par, keep, mi, ready, store, send, wait_rows):
        nr = rows // 128

        def build(i, gm):
            rs = pl.ds(pl.multiple_of(i * CHUNK, CHUNK), CHUNK)
            m = jnp.transpose(mb[mi, :, rs])
            for half, owner in enumerate((me, part)):
                base = (owner * rows).astype(f32)
                for c in range(nr):
                    rid = lane_col + (base + c * 128.0)
                    g = jnp.where(m[:, 0:1] == rid, m[:, 8:9], 0.0)
                    for k in range(1, top_k):
                        g = jnp.where(m[:, k:k + 1] == rid, m[:, 8 + k:9 + k], g)
                    g1 = g.astype(bf16)
                    rem = g - g1.astype(f32)
                    g2 = rem.astype(bf16)
                    g3 = (rem - g2.astype(f32)).astype(bf16)
                    lanes = slice(half * rows + c * 128, half * rows + c * 128 + 128)
                    gm[0, :, lanes] = g1
                    gm[1, :, lanes] = g2
                    gm[2, :, lanes] = g3

        def products(i, gm):
            rs = pl.ds(pl.multiple_of(i * CHUNK, CHUNK), CHUNK)
            for n in range(hidden // 256):
                cols = slice(n * 256, n * 256 + 256)
                v = None
                for q in range(3):
                    t = dot(gm[q, :, 0:rows], r_mine[keep, :, cols]) + dot(gm[q, :, rows:], r_in[par, :, cols])
                    v = t if v is None else v + t
                store(rs, cols, v + v)

        build(jnp.int32(0), gma)
        wait_rows()

        def pair(j, _):
            for t, (now, later) in enumerate(((gma, gmb), (gmb, gma))):
                i = 2 * j + t
                rs = pl.ds(pl.multiple_of(i * CHUNK, CHUNK), CHUNK)
                ready(i, rs)
                build((i + 1) % chunks, later)
                products(i, now)
                send(i, rs)
            return 0
        lax.fori_loop(0, chunks // 2, pair, 0)

    def chunk_rows(c):
        return pl.ds(c * CHUNK, CHUNK)

    def s_copy(which, c, rs):
        src, dst, dev = ((s1, got1, n1), (sd, gotd, n1), (s1, got2, n2))[which]
        return remote(src.at[rs], dst.at[rs], s_send.at[which, c], s_recv.at[which, c], dev)

    def put_s1(rs, cols, v):
        s1[rs, cols] = v

    def put_sd(rs, cols, v):
        sd[rs, cols] = v

    def put_s2(rs, cols, v):
        s1[rs, cols] = v + gotd[rs, cols]

    def nothing(i, rs):
        pass

    def first_tokens():
        t_n1.wait_recv()
        t_d.start()
        t_n1p.start()
        t_n2.start()

    t_own.wait_recv()
    expert_loop(0, 2, 1, tok_ref, tb.at[0], 7, 0, late=((local - 3, t_head.start), (local - 1, first_tokens)))
    t_n1p.wait_recv()
    whole_rows(2).wait_send()

    expert_loop(1, 0, 0, tb.at[1], tb.at[2], 1, 2)
    t_d.wait_recv()
    t_dp.start()
    combine(0, 0, 1, nothing, put_s1, lambda i, rs: s_copy(0, i, rs).start(), lambda: whole_rows(0).wait())
    t_dp.wait_recv()

    expert_loop(2, 1, 0, tb.at[3], tb.at[4], 3, 4)
    t_head.wait_recv()
    t_n2.wait_recv()
    t_n2p.start()
    combine(1, 0, 3, nothing, put_sd, lambda i, rs: s_copy(1, i, rs).start(), lambda: whole_rows(1).wait())
    t_n2p.wait_recv()

    expert_loop(3, 0, 0, tb.at[5], tb.at[6], 5, 6)
    for c in range(chunks):
        s_copy(0, c, chunk_rows(c)).wait_send()
    combine(0, 0, 5, lambda i, rs: s_copy(1, i, rs).wait_recv(), put_s2, lambda i, rs: s_copy(2, i, rs).start(),
            lambda: whole_rows(0).wait())

    for c in range(chunks):
        s_copy(1, c, chunk_rows(c)).wait_send()
    combine(2, 1, 7, nothing, put_sd, nothing, lambda: whole_rows(2).wait_recv())

    mrows = 256
    for s in range(2):
        slot = (4 * local + s) % SLOTS
        wait_weights(slot)

        def block(i, _):
            rs = pl.ds(pl.multiple_of(i * mrows, mrows), mrows)

            def put(cols, v):
                h_ref[:, cols] = v
            swiglu_up(tok_ref[rs, :], slot, put)
            logit = jnp.sum(tok_ref[rs, :].astype(f32) * gate_ref[...].astype(f32).reshape(1, hidden), axis=1, keepdims=True)
            sig = jax.nn.sigmoid(logit)
            for n in range(hidden // 256):
                cols = slice(n * 256, n * 256 + 256)
                v = sd[rs, cols] + sig * dot(h_ref[...], w2s[slot, :, cols])
                if s == 1:
                    v = v + tok_ref[rs, cols].astype(f32)
                sd[rs, cols] = v
            return 0
        lax.fori_loop(0, tok_count // mrows, block, 0)

    for c in range(chunks):
        rs = chunk_rows(c)
        s_copy(0, c, rs).wait_recv()
        s_copy(2, c, rs).wait_recv()
        out_ref[rs, :] = (sd[rs, :] + got1[rs, :] + got2[rs, :]).astype(bf16)
        pltpu.make_async_copy(out_ref.at[rs], out_hbm.at[rs], o_sem.at[c]).start()
    for c in range(chunks):
        rs = chunk_rows(c)
        s_copy(2, c, rs).wait_send()
        pltpu.make_async_copy(out_ref.at[rs], out_hbm.at[rs], o_sem.at[c]).wait()
    for t in (t_head, t_own, t_n1, t_n1p, t_d, t_dp, t_n2, t_n2p):
        t.wait_send()


def solution(mesh):
    num_ep = mesh.shape['ep']
    row_spec = P(('dp', 'ep'), None)
    replicated = P()
    expert_spec = P('ep', None, None)

    def device_step(tokens, expert_ids, gate_vals, slots, shared_w1, shared_w3, shared_w2, shared_gate, expert_w1, expert_w3, expert_w2):
        tok_count, hidden = tokens.shape
        top_k = expert_ids.shape[1]
        local, _, ff = expert_w1.shape
        num_experts = local * num_ep
        cap = 8 * ((2 * tok_count * top_k + 8 * num_experts - 1) // (8 * num_experts))
        rows = local * cap
        chunks = tok_count // CHUNK
        vm = pl.BlockSpec(memory_space=pltpu.VMEM)
        hbm = pl.BlockSpec(memory_space=pltpu.HBM)
        dma = pltpu.SemaphoreType.DMA
        return pl.pallas_call(
            functools.partial(moe_kernel, num_ep, local, cap, top_k),
            out_shape=jax.ShapeDtypeStruct((tok_count, hidden), bf16),
            in_specs=[hbm] * 4 + [vm] + [hbm] * 6,
            out_specs=hbm,
            scratch_shapes=[
                pltpu.VMEM((tok_count, hidden), bf16),
                pltpu.VMEM((tok_count, hidden), bf16),
                pltpu.VMEM((top_k, tok_count), jnp.int32),
                pltpu.VMEM((top_k, tok_count), jnp.int32),
                pltpu.VMEM((top_k, tok_count), f32),
                pltpu.VMEM((7, tok_count, hidden), bf16),
                pltpu.VMEM((8, 16, tok_count), f32),
                pltpu.VMEM((2, rows, hidden), bf16),
                pltpu.VMEM((rows, hidden), bf16),
                pltpu.VMEM((3, rows, hidden), bf16),
                pltpu.VMEM((SLOTS, hidden, ff), bf16),
                pltpu.VMEM((SLOTS, hidden, ff), bf16),
                pltpu.VMEM((SLOTS, ff, hidden), bf16),
            ] + [pltpu.VMEM((tok_count, hidden), f32)] * 5 + [
                pltpu.VMEM((256, ff), bf16),
                pltpu.VMEM((2 * cap, hidden), bf16),
                pltpu.VMEM((3, CHUNK, 2 * rows), bf16),
                pltpu.VMEM((3, CHUNK, 2 * rows), bf16),
                dma((4,)), dma((chunks,)), dma((SLOTS, 3)), dma((8,)), dma((8,)), dma((7,)), dma((7,)),
                dma, dma((3,)), dma((3, chunks)), dma((3, chunks)),
            ],
            compiler_params=pltpu.CompilerParams(collective_id=0, has_side_effects=True, vmem_limit_bytes=67043328),
        )(expert_ids.T, slots.T, gate_vals.T, tokens, shared_gate, shared_w1, shared_w3, shared_w2, expert_w1, expert_w3, expert_w2)

    return jax.shard_map(device_step, mesh=mesh, in_specs=(row_spec, row_spec, row_spec, row_spec, replicated, replicated, replicated, replicated, expert_spec, expert_spec, expert_spec), out_specs=row_spec, check_vma=False)
```

```python
import functools

import jax
import jax.numpy as jnp
from jax import lax
from jax.experimental import pallas as pl
from jax.experimental.pallas import tpu as pltpu
from jax.sharding import PartitionSpec as P

SLOTS = 3
CHUNK = 128
HEAD = 256
f32, bf16 = jnp.float32, jnp.bfloat16


def dot(a, b):
    return jnp.dot(a, b, preferred_element_type=f32)


def moe_kernel(num_ep, local, cap, top_k, ids_hbm, slot_hbm, gval_hbm, tok_hbm, gate_ref, sw1, sw3, sw2, ew1, ew3, ew2, out_ref,
               tok_ref, ids_ref, slot_ref, gval_ref, tb, mb, r_mine, r_out, r_in, w1s, w3s, w2s, s1, sd, got1, gotd, got2, h_ref, xs, gma, gmb,
               i_sem, w_sem, t_send, t_recv, m_send, m_recv, r_send, r_recv, s_send, s_recv):
    tok_count, hidden = tok_ref.shape
    ff = w1s.shape[2]
    rows = local * cap
    chunks = tok_count // CHUNK
    me = lax.axis_index('ep')
    core, xx, yy = me % 2, (me // 2) % 2, me // 4
    step_x, step_y = 2 - 4 * xx, 4 - 8 * yy
    part = me + 1 - 2 * core
    n1 = me + (1 - core) * step_x + core * step_y
    n2 = me + core * step_x + (1 - core) * step_y

    def remote(src, dst, ss, rs, dev):
        return pltpu.make_async_remote_copy(src_ref=src, dst_ref=dst, send_sem=ss, recv_sem=rs,
                                            device_id={'ep': dev}, device_id_type=pl.DeviceIdType.MESH)

    def weight_copies(src1, src3, src2, slot):
        return [pltpu.make_async_copy(src1, w1s.at[slot], w_sem.at[slot, 0]),
                pltpu.make_async_copy(src3, w3s.at[slot], w_sem.at[slot, 1]),
                pltpu.make_async_copy(src2, w2s.at[slot], w_sem.at[slot, 2])]

    def start_expert(e, slot):
        for c in weight_copies(ew1.at[e], ew3.at[e], ew2.at[e], slot):
            c.start()

    def start_shared(s, slot):
        cols = pl.ds(s * ff, ff)
        for c in weight_copies(sw1.at[:, cols], sw3.at[:, cols], sw2.at[cols, :], slot):
            c.start()

    def wait_weights(slot):
        for c in weight_copies(ew1.at[0], ew3.at[0], ew2.at[0], slot):
            c.wait()

    barrier = pltpu.get_barrier_semaphore()
    for dev in (n1, n2, part):
        pl.semaphore_signal(barrier, inc=1, device_id={'ep': dev}, device_id_type=pl.DeviceIdType.MESH)
    loads = [pltpu.make_async_copy(src, dst, i_sem.at[k]) for k, (src, dst) in enumerate((
        (ids_hbm, ids_ref), (slot_hbm, slot_ref), (gval_hbm, gval_ref), (tok_hbm, tok_ref)))]
    for c in loads:
        c.start()
    loads[3].wait()
    pl.semaphore_wait(barrier, 3)

    class Hop:
        def __init__(self, src, dst, dev):
            self.copies = (remote(mb.at[src], mb.at[dst], m_send.at[dst], m_recv.at[dst], dev),
                           remote(tok_ref if src == 7 else tb.at[src], tb.at[dst], t_send.at[dst], t_recv.at[dst], dev))

        def start(self):
            for c in self.copies:
                c.start()

        def wait_recv(self):
            for c in self.copies:
                c.wait_recv()

        def wait_send(self):
            for c in self.copies:
                c.wait_send()

    t_own, t_n1, t_n1p, t_d, t_dp, t_n2, t_n2p = (
        Hop(7, 0, part), Hop(7, 1, n1), Hop(1, 2, part), Hop(1, 3, n2), Hop(3, 4, part), Hop(7, 5, n2), Hop(5, 6, part))
    head, tail = pl.ds(0, HEAD), pl.ds(HEAD, tok_count - HEAD)
    t_head = remote(tok_ref.at[head], tb.at[5, head], t_send.at[7], t_recv.at[7], n2)
    t_n2.copies = (t_n2.copies[0], remote(tok_ref.at[tail], tb.at[5, tail], t_send.at[5], t_recv.at[5], n2))
    t_n1.copies[1].start()
    t_own.copies[1].start()
    for c in loads[:3]:
        c.wait()
    for e in range(SLOTS):
        start_expert(e, e)

    kept = slot_ref[...] >= 0
    mb[7, 0:top_k, :] = jnp.where(kept, ids_ref[...] * cap + slot_ref[...], -1).astype(f32)
    mb[7, top_k:8, :] = jnp.full((8 - top_k, tok_count), -1.0, f32)
    mb[7, 8:8 + top_k, :] = jnp.where(kept, 0.5 * gval_ref[...], 0.0)
    mb[7, 8 + top_k:16, :] = jnp.zeros((8 - top_k, tok_count), f32)

    t_n1.copies[0].start()
    t_own.copies[0].start()

    def swiglu_up(x, slot, put):
        full = ff // 256
        for c in range(full):
            cols = slice(c * 256, c * 256 + 256)
            a = dot(x, w1s[slot, :, cols])
            b = dot(x, w3s[slot, :, cols])
            put(cols, (jax.nn.silu(a) * b).astype(bf16))
        cols = slice(full * 256, ff)
        rest = ff - full * 256
        ab = dot(x, jnp.concatenate([w1s[slot, :, cols], w3s[slot, :, cols]], axis=1))
        put(cols, (jax.nn.silu(ab[:, :rest]) * ab[:, rest:]).astype(bf16))

    lane_row = lax.broadcasted_iota(jnp.int32, (cap, tok_count), 0).astype(f32)
    lane_col = lax.broadcasted_iota(jnp.int32, (CHUNK, 128), 1).astype(f32)

    def whole_rows(par):
        return remote(r_out, r_in.at[par], r_send, r_recv.at[par], part)

    def expert_loop(order, par, keep, mine, other, mi, oi, late=()):
        def dispatch(e):
            base = ((me * local + e) * cap).astype(f32)
            for u, (unit, who) in enumerate(((mine, mi), (other, oi))):
                d = mb[who, 0:8, :] - base
                hit = d[0:1, :] == lane_row
                for k in range(1, top_k):
                    hit = hit | (d[k:k + 1, :] == lane_row)
                pick = jnp.where(hit, 1.0, 0.0).astype(bf16)
                for n in range(hidden // 256):
                    cols = slice(n * 256, n * 256 + 256)
                    xs[u * cap:(u + 1) * cap, cols] = dot(pick, unit[:, cols]).astype(bf16)

        dispatch(jnp.int32(0))

        def body(e, _):
            for at, what in late:
                pl.when(e == at)(what)
            slot = (order * local + e) % SLOTS
            wait_weights(slot)

            def put(cols, v):
                h_ref[0:2 * cap, cols] = v
            swiglu_up(xs[...], slot, put)
            dispatch(e + 1)
            rs = pl.ds(pl.multiple_of(e * cap, cap), cap)
            for n in range(hidden // 256):
                cols = slice(n * 256, n * 256 + 256)
                v = dot(h_ref[0:2 * cap, :], w2s[slot, :, cols]).astype(bf16)
                r_mine[keep, rs, cols] = v[:cap]
                r_out[rs, cols] = v[cap:]
            remote(r_out.at[rs], r_in.at[par, rs], r_send, r_recv.at[par], part).start()
            if order < 3:
                start_expert((e + SLOTS) % local, slot)
            else:
                @pl.when(e + SLOTS < local)
                def _():
                    start_expert(e + SLOTS, slot)
                for s in range(2):
                    @pl.when(e + SLOTS == local + s)
                    def _():
                        start_shared(s, slot)
            return 0
        lax.fori_loop(0, local, body, 0)

    def combine(par, keep, mi, ready, store, send, wait_rows):
        nr = rows // 128

        def build(i, gm):
            rs = pl.ds(pl.multiple_of(i * CHUNK, CHUNK), CHUNK)
            m = jnp.transpose(mb[mi, :, rs])
            for half, owner in enumerate((me, part)):
                base = (owner * rows).astype(f32)
                for c in range(nr):
                    rid = lane_col + (base + c * 128.0)
                    g = jnp.where(m[:, 0:1] == rid, m[:, 8:9], 0.0)
                    for k in range(1, top_k):
                        g = jnp.where(m[:, k:k + 1] == rid, m[:, 8 + k:9 + k], g)
                    g1 = g.astype(bf16)
                    rem = g - g1.astype(f32)
                    g2 = rem.astype(bf16)
                    g3 = (rem - g2.astype(f32)).astype(bf16)
                    lanes = slice(half * rows + c * 128, half * rows + c * 128 + 128)
                    gm[0, :, lanes] = g1
                    gm[1, :, lanes] = g2
                    gm[2, :, lanes] = g3

        def products(i, gm):
            rs = pl.ds(pl.multiple_of(i * CHUNK, CHUNK), CHUNK)
            for n in range(hidden // 256):
                cols = slice(n * 256, n * 256 + 256)
                v = None
                for q in range(3):
                    t = dot(gm[q, :, 0:rows], r_mine[keep, :, cols]) + dot(gm[q, :, rows:], r_in[par, :, cols])
                    v = t if v is None else v + t
                store(rs, cols, v + v)

        build(jnp.int32(0), gma)
        wait_rows()

        def pair(j, _):
            for t, (now, later) in enumerate(((gma, gmb), (gmb, gma))):
                i = 2 * j + t
                rs = pl.ds(pl.multiple_of(i * CHUNK, CHUNK), CHUNK)
                ready(i, rs)
                build((i + 1) % chunks, later)
                products(i, now)
                send(i, rs)
            return 0
        lax.fori_loop(0, chunks // 2, pair, 0)

    def chunk_rows(c):
        return pl.ds(c * CHUNK, CHUNK)

    def s_copy(which, c, rs):
        src, dst, dev = ((s1, got1, n1), (sd, gotd, n1), (s1, got2, n2))[which]
        return remote(src.at[rs], dst.at[rs], s_send.at[which, c], s_recv.at[which, c], dev)

    def put_s1(rs, cols, v):
        s1[rs, cols] = v

    def put_sd(rs, cols, v):
        sd[rs, cols] = v

    def put_s2(rs, cols, v):
        s1[rs, cols] = v + gotd[rs, cols]

    def nothing(i, rs):
        pass

    def first_tokens():
        t_n1.wait_recv()
        t_d.start()
        t_n1p.start()
        t_n2.start()

    t_own.wait_recv()
    expert_loop(0, 2, 1, tok_ref, tb.at[0], 7, 0, late=((local - 3, t_head.start), (local - 1, first_tokens)))
    t_n1p.wait_recv()
    whole_rows(2).wait_send()

    expert_loop(1, 0, 0, tb.at[1], tb.at[2], 1, 2)
    t_d.wait_recv()
    t_dp.start()
    combine(0, 0, 1, nothing, put_s1, lambda i, rs: s_copy(0, i, rs).start(), lambda: whole_rows(0).wait())
    t_dp.wait_recv()

    expert_loop(2, 1, 0, tb.at[3], tb.at[4], 3, 4)
    t_head.wait_recv()
    t_n2.wait_recv()
    t_n2p.start()
    combine(1, 0, 3, nothing, put_sd, lambda i, rs: s_copy(1, i, rs).start(), lambda: whole_rows(1).wait())
    t_n2p.wait_recv()

    expert_loop(3, 0, 0, tb.at[5], tb.at[6], 5, 6)
    for c in range(chunks):
        s_copy(0, c, chunk_rows(c)).wait_send()
    combine(0, 0, 5, lambda i, rs: s_copy(1, i, rs).wait_recv(), put_s2, lambda i, rs: s_copy(2, i, rs).start(),
            lambda: whole_rows(0).wait())

    for c in range(chunks):
        s_copy(1, c, chunk_rows(c)).wait_send()
    combine(2, 1, 7, nothing, put_sd, nothing, lambda: whole_rows(2).wait_recv())

    mrows = 256
    for s in range(2):
        slot = (4 * local + s) % SLOTS
        wait_weights(slot)

        def block(i, _):
            rs = pl.ds(pl.multiple_of(i * mrows, mrows), mrows)

            def put(cols, v):
                h_ref[:, cols] = v
            swiglu_up(tok_ref[rs, :], slot, put)
            logit = jnp.sum(tok_ref[rs, :].astype(f32) * gate_ref[...].astype(f32).reshape(1, hidden), axis=1, keepdims=True)
            sig = jax.nn.sigmoid(logit)
            for n in range(hidden // 256):
                cols = slice(n * 256, n * 256 + 256)
                v = sd[rs, cols] + sig * dot(h_ref[...], w2s[slot, :, cols])
                if s == 1:
                    v = v + tok_ref[rs, cols].astype(f32)
                sd[rs, cols] = v
            return 0
        lax.fori_loop(0, tok_count // mrows, block, 0)

    for c in range(chunks):
        rs = chunk_rows(c)
        s_copy(0, c, rs).wait_recv()
        s_copy(2, c, rs).wait_recv()
        out_ref[rs, :] = (sd[rs, :] + got1[rs, :] + got2[rs, :]).astype(bf16)
    for c in range(chunks):
        rs = chunk_rows(c)
        s_copy(2, c, rs).wait_send()
    for t in (t_head, t_own, t_n1, t_n1p, t_d, t_dp, t_n2, t_n2p):
        t.wait_send()


def solution(mesh):
    num_ep = mesh.shape['ep']
    row_spec = P(('dp', 'ep'), None)
    replicated = P()
    expert_spec = P('ep', None, None)

    def device_step(tokens, expert_ids, gate_vals, slots, shared_w1, shared_w3, shared_w2, shared_gate, expert_w1, expert_w3, expert_w2):
        tok_count, hidden = tokens.shape
        top_k = expert_ids.shape[1]
        local, _, ff = expert_w1.shape
        num_experts = local * num_ep
        cap = 8 * ((2 * tok_count * top_k + 8 * num_experts - 1) // (8 * num_experts))
        rows = local * cap
        chunks = tok_count // CHUNK
        vm = pl.BlockSpec(memory_space=pltpu.VMEM)
        hbm = pl.BlockSpec(memory_space=pltpu.HBM)
        dma = pltpu.SemaphoreType.DMA
        return pl.pallas_call(
            functools.partial(moe_kernel, num_ep, local, cap, top_k),
            out_shape=pltpu.VMEM((tok_count, hidden), bf16),
            in_specs=[hbm] * 4 + [vm] + [hbm] * 6,
            out_specs=vm,
            scratch_shapes=[
                pltpu.VMEM((tok_count, hidden), bf16),
                pltpu.VMEM((top_k, tok_count), jnp.int32),
                pltpu.VMEM((top_k, tok_count), jnp.int32),
                pltpu.VMEM((top_k, tok_count), f32),
                pltpu.VMEM((7, tok_count, hidden), bf16),
                pltpu.VMEM((8, 16, tok_count), f32),
                pltpu.VMEM((2, rows, hidden), bf16),
                pltpu.VMEM((rows, hidden), bf16),
                pltpu.VMEM((3, rows, hidden), bf16),
                pltpu.VMEM((SLOTS, hidden, ff), bf16),
                pltpu.VMEM((SLOTS, hidden, ff), bf16),
                pltpu.VMEM((SLOTS, ff, hidden), bf16),
            ] + [pltpu.VMEM((tok_count, hidden), f32)] * 5 + [
                pltpu.VMEM((256, ff), bf16),
                pltpu.VMEM((2 * cap, hidden), bf16),
                pltpu.VMEM((3, CHUNK, 2 * rows), bf16),
                pltpu.VMEM((3, CHUNK, 2 * rows), bf16),
                dma((4,)), dma((SLOTS, 3)), dma((8,)), dma((8,)), dma((7,)), dma((7,)),
                dma, dma((3,)), dma((3, chunks)), dma((3, chunks)),
            ],
            compiler_params=pltpu.CompilerParams(collective_id=0, has_side_effects=True, vmem_limit_bytes=64000000),
        )(expert_ids.T, slots.T, gate_vals.T, tokens, shared_gate, shared_w1, shared_w3, shared_w2, expert_w1, expert_w3, expert_w2)

    return jax.shard_map(device_step, mesh=mesh, in_specs=(row_spec, row_spec, row_spec, row_spec, replicated, replicated, replicated, replicated, expert_spec, expert_spec, expert_spec), out_specs=row_spec, check_vma=False)
```

```python
import functools

import jax
import jax.numpy as jnp
from jax import lax
from jax.experimental import pallas as pl
from jax.experimental.pallas import tpu as pltpu
from jax.sharding import PartitionSpec as P

SLOTS = 3
CHUNK = 128
HEAD = 256
f32, bf16 = jnp.float32, jnp.bfloat16


def dot(a, b):
    return jnp.dot(a, b, preferred_element_type=f32)


def moe_kernel(num_ep, local, cap, top_k, ids_hbm, slot_hbm, gval_hbm, tok_hbm, gate_hbm, sw1, sw3, sw2, ew1, ew3, ew2, out_ref,
               tok_ref, ids_ref, slot_ref, gval_ref, gate_ref, tb, mb, r_mine, r_out, r_in, w1s, w3s, w2s, s1, sd, got1, gotd, got2, h_ref, xs, gma, gmb,
               i_sem, w_sem, t_send, t_recv, m_send, m_recv, r_send, r_recv, s_send, s_recv):
    tok_count, hidden = tok_ref.shape
    ff = w1s.shape[2]
    rows = local * cap
    chunks = tok_count // CHUNK
    me = lax.axis_index('ep')
    core, xx, yy = me % 2, (me // 2) % 2, me // 4
    step_x, step_y = 2 - 4 * xx, 4 - 8 * yy
    part = me + 1 - 2 * core
    n1 = me + (1 - core) * step_x + core * step_y
    n2 = me + core * step_x + (1 - core) * step_y

    def remote(src, dst, ss, rs, dev):
        return pltpu.make_async_remote_copy(src_ref=src, dst_ref=dst, send_sem=ss, recv_sem=rs,
                                            device_id={'ep': dev}, device_id_type=pl.DeviceIdType.MESH)

    def weight_copies(src1, src3, src2, slot):
        return [pltpu.make_async_copy(src1, w1s.at[slot], w_sem.at[slot, 0]),
                pltpu.make_async_copy(src3, w3s.at[slot], w_sem.at[slot, 1]),
                pltpu.make_async_copy(src2, w2s.at[slot], w_sem.at[slot, 2])]

    def start_expert(e, slot):
        for c in weight_copies(ew1.at[e], ew3.at[e], ew2.at[e], slot):
            c.start()

    def start_shared(s, slot):
        cols = pl.ds(s * ff, ff)
        for c in weight_copies(sw1.at[:, cols], sw3.at[:, cols], sw2.at[cols, :], slot):
            c.start()

    def wait_weights(slot):
        for c in weight_copies(ew1.at[0], ew3.at[0], ew2.at[0], slot):
            c.wait()

    barrier = pltpu.get_barrier_semaphore()
    for dev in (n1, n2, part):
        pl.semaphore_signal(barrier, inc=1, device_id={'ep': dev}, device_id_type=pl.DeviceIdType.MESH)
    loads = [pltpu.make_async_copy(src, dst, i_sem.at[k]) for k, (src, dst) in enumerate((
        (ids_hbm, ids_ref), (slot_hbm, slot_ref), (gval_hbm, gval_ref), (tok_hbm, tok_ref), (gate_hbm, gate_ref)))]
    for c in loads:
        c.start()
    loads[3].wait()
    pl.semaphore_wait(barrier, 3)

    class Hop:
        def __init__(self, src, dst, dev):
            self.copies = (remote(mb.at[src], mb.at[dst], m_send.at[dst], m_recv.at[dst], dev),
                           remote(tok_ref if src == 7 else tb.at[src], tb.at[dst], t_send.at[dst], t_recv.at[dst], dev))

        def start(self):
            for c in self.copies:
                c.start()

        def wait_recv(self):
            for c in self.copies:
                c.wait_recv()

        def wait_send(self):
            for c in self.copies:
                c.wait_send()

    t_own, t_n1, t_n1p, t_d, t_dp, t_n2, t_n2p = (
        Hop(7, 0, part), Hop(7, 1, n1), Hop(1, 2, part), Hop(1, 3, n2), Hop(3, 4, part), Hop(7, 5, n2), Hop(5, 6, part))
    head, tail = pl.ds(0, HEAD), pl.ds(HEAD, tok_count - HEAD)
    t_head = remote(tok_ref.at[head], tb.at[5, head], t_send.at[7], t_recv.at[7], n2)
    t_n2.copies = (t_n2.copies[0], remote(tok_ref.at[tail], tb.at[5, tail], t_send.at[5], t_recv.at[5], n2))
    t_n1.copies[1].start()
    t_own.copies[1].start()
    for c in loads[:3] + loads[4:]:
        c.wait()
    for e in range(SLOTS):
        start_expert(e, e)

    kept = slot_ref[...] >= 0
    mb[7, 0:top_k, :] = jnp.where(kept, ids_ref[...] * cap + slot_ref[...], -1).astype(f32)
    mb[7, top_k:8, :] = jnp.full((8 - top_k, tok_count), -1.0, f32)
    mb[7, 8:8 + top_k, :] = jnp.where(kept, 0.5 * gval_ref[...], 0.0)
    mb[7, 8 + top_k:16, :] = jnp.zeros((8 - top_k, tok_count), f32)

    t_n1.copies[0].start()
    t_own.copies[0].start()

    def swiglu_up(x, slot, put):
        full = ff // 256
        for c in range(full):
            cols = slice(c * 256, c * 256 + 256)
            a = dot(x, w1s[slot, :, cols])
            b = dot(x, w3s[slot, :, cols])
            put(cols, (jax.nn.silu(a) * b).astype(bf16))
        cols = slice(full * 256, ff)
        rest = ff - full * 256
        ab = dot(x, jnp.concatenate([w1s[slot, :, cols], w3s[slot, :, cols]], axis=1))
        put(cols, (jax.nn.silu(ab[:, :rest]) * ab[:, rest:]).astype(bf16))

    lane_row = lax.broadcasted_iota(jnp.int32, (cap, tok_count), 0).astype(f32)
    lane_col = lax.broadcasted_iota(jnp.int32, (CHUNK, 128), 1).astype(f32)

    def whole_rows(par):
        return remote(r_out, r_in.at[par], r_send, r_recv.at[par], part)

    def expert_loop(order, par, keep, mine, other, mi, oi, late=()):
        def dispatch(e):
            base = ((me * local + e) * cap).astype(f32)
            for u, (unit, who) in enumerate(((mine, mi), (other, oi))):
                d = mb[who, 0:8, :] - base
                hit = d[0:1, :] == lane_row
                for k in range(1, top_k):
                    hit = hit | (d[k:k + 1, :] == lane_row)
                pick = jnp.where(hit, 1.0, 0.0).astype(bf16)
                for n in range(hidden // 256):
                    cols = slice(n * 256, n * 256 + 256)
                    xs[u * cap:(u + 1) * cap, cols] = dot(pick, unit[:, cols]).astype(bf16)

        dispatch(jnp.int32(0))

        def body(e, _):
            for at, what in late:
                pl.when(e == at)(what)
            slot = (order * local + e) % SLOTS
            wait_weights(slot)

            def put(cols, v):
                h_ref[0:2 * cap, cols] = v
            swiglu_up(xs[...], slot, put)
            dispatch(e + 1)
            rs = pl.ds(pl.multiple_of(e * cap, cap), cap)
            for n in range(hidden // 256):
                cols = slice(n * 256, n * 256 + 256)
                v = dot(h_ref[0:2 * cap, :], w2s[slot, :, cols]).astype(bf16)
                r_mine[keep, rs, cols] = v[:cap]
                r_out[rs, cols] = v[cap:]
            remote(r_out.at[rs], r_in.at[par, rs], r_send, r_recv.at[par], part).start()
            if order < 3:
                start_expert((e + SLOTS) % local, slot)
            else:
                @pl.when(e + SLOTS < local)
                def _():
                    start_expert(e + SLOTS, slot)
                for s in range(2):
                    @pl.when(e + SLOTS == local + s)
                    def _():
                        start_shared(s, slot)
            return 0
        lax.fori_loop(0, local, body, 0)

    def combine(par, keep, mi, ready, store, send, wait_rows):
        nr = rows // 128

        def build(i, gm):
            rs = pl.ds(pl.multiple_of(i * CHUNK, CHUNK), CHUNK)
            m = jnp.transpose(mb[mi, :, rs])
            for half, owner in enumerate((me, part)):
                base = (owner * rows).astype(f32)
                for c in range(nr):
                    rid = lane_col + (base + c * 128.0)
                    g = jnp.where(m[:, 0:1] == rid, m[:, 8:9], 0.0)
                    for k in range(1, top_k):
                        g = jnp.where(m[:, k:k + 1] == rid, m[:, 8 + k:9 + k], g)
                    g1 = g.astype(bf16)
                    rem = g - g1.astype(f32)
                    g2 = rem.astype(bf16)
                    g3 = (rem - g2.astype(f32)).astype(bf16)
                    lanes = slice(half * rows + c * 128, half * rows + c * 128 + 128)
                    gm[0, :, lanes] = g1
                    gm[1, :, lanes] = g2
                    gm[2, :, lanes] = g3

        def products(i, gm):
            rs = pl.ds(pl.multiple_of(i * CHUNK, CHUNK), CHUNK)
            for n in range(hidden // 256):
                cols = slice(n * 256, n * 256 + 256)
                v = None
                for q in range(3):
                    t = dot(gm[q, :, 0:rows], r_mine[keep, :, cols]) + dot(gm[q, :, rows:], r_in[par, :, cols])
                    v = t if v is None else v + t
                store(rs, cols, v + v)

        build(jnp.int32(0), gma)
        wait_rows()

        def pair(j, _):
            for t, (now, later) in enumerate(((gma, gmb), (gmb, gma))):
                i = 2 * j + t
                rs = pl.ds(pl.multiple_of(i * CHUNK, CHUNK), CHUNK)
                ready(i, rs)
                build((i + 1) % chunks, later)
                products(i, now)
                send(i, rs)
            return 0
        lax.fori_loop(0, chunks // 2, pair, 0)

    def chunk_rows(c):
        return pl.ds(c * CHUNK, CHUNK)

    def s_copy(which, c, rs):
        src, dst, dev = ((s1, got1, n1), (sd, gotd, n1), (s1, got2, n2))[which]
        return remote(src.at[rs], dst.at[rs], s_send.at[which, c], s_recv.at[which, c], dev)

    def put_s1(rs, cols, v):
        s1[rs, cols] = v

    def put_sd(rs, cols, v):
        sd[rs, cols] = v

    def put_s2(rs, cols, v):
        s1[rs, cols] = v + gotd[rs, cols]

    def nothing(i, rs):
        pass

    def first_tokens():
        t_n1.wait_recv()
        t_d.start()
        t_n1p.start()
        t_n2.start()

    t_own.wait_recv()
    expert_loop(0, 2, 1, tok_ref, tb.at[0], 7, 0, late=((local - 3, t_head.start), (local - 1, first_tokens)))
    t_n1p.wait_recv()
    whole_rows(2).wait_send()

    expert_loop(1, 0, 0, tb.at[1], tb.at[2], 1, 2)
    t_d.wait_recv()
    t_dp.start()
    combine(0, 0, 1, nothing, put_s1, lambda i, rs: s_copy(0, i, rs).start(), lambda: whole_rows(0).wait())
    t_dp.wait_recv()

    expert_loop(2, 1, 0, tb.at[3], tb.at[4], 3, 4)
    t_head.wait_recv()
    t_n2.wait_recv()
    t_n2p.start()
    combine(1, 0, 3, nothing, put_sd, lambda i, rs: s_copy(1, i, rs).start(), lambda: whole_rows(1).wait())
    t_n2p.wait_recv()

    expert_loop(3, 0, 0, tb.at[5], tb.at[6], 5, 6)
    for c in range(chunks):
        s_copy(0, c, chunk_rows(c)).wait_send()
    combine(0, 0, 5, lambda i, rs: s_copy(1, i, rs).wait_recv(), put_s2, lambda i, rs: s_copy(2, i, rs).start(),
            lambda: whole_rows(0).wait())

    for c in range(chunks):
        s_copy(1, c, chunk_rows(c)).wait_send()
    combine(2, 1, 7, nothing, put_sd, nothing, lambda: whole_rows(2).wait_recv())

    mrows = 256
    for s in range(2):
        slot = (4 * local + s) % SLOTS
        wait_weights(slot)

        def block(i, _):
            rs = pl.ds(pl.multiple_of(i * mrows, mrows), mrows)

            def put(cols, v):
                h_ref[:, cols] = v
            swiglu_up(tok_ref[rs, :], slot, put)
            logit = jnp.sum(tok_ref[rs, :].astype(f32) * gate_ref[...].astype(f32).reshape(1, hidden), axis=1, keepdims=True)
            sig = jax.nn.sigmoid(logit)
            for n in range(hidden // 256):
                cols = slice(n * 256, n * 256 + 256)
                v = sd[rs, cols] + sig * dot(h_ref[...], w2s[slot, :, cols])
                if s == 1:
                    v = v + tok_ref[rs, cols].astype(f32)
                sd[rs, cols] = v
            return 0
        lax.fori_loop(0, tok_count // mrows, block, 0)

    for c in range(chunks):
        rs = chunk_rows(c)
        s_copy(0, c, rs).wait_recv()
        s_copy(2, c, rs).wait_recv()
        out_ref[rs, :] = (sd[rs, :] + got1[rs, :] + got2[rs, :]).astype(bf16)
    for c in range(chunks):
        rs = chunk_rows(c)
        s_copy(2, c, rs).wait_send()
    for t in (t_head, t_own, t_n1, t_n1p, t_d, t_dp, t_n2, t_n2p):
        t.wait_send()


def solution(mesh):
    num_ep = mesh.shape['ep']
    row_spec = P(('dp', 'ep'), None)
    replicated = P()
    expert_spec = P('ep', None, None)

    def device_step(tokens, expert_ids, gate_vals, slots, shared_w1, shared_w3, shared_w2, shared_gate, expert_w1, expert_w3, expert_w2):
        tok_count, hidden = tokens.shape
        top_k = expert_ids.shape[1]
        local, _, ff = expert_w1.shape
        num_experts = local * num_ep
        cap = 8 * ((2 * tok_count * top_k + 8 * num_experts - 1) // (8 * num_experts))
        rows = local * cap
        chunks = tok_count // CHUNK
        vm = pl.BlockSpec(memory_space=pltpu.VMEM)
        hbm = pl.BlockSpec(memory_space=pltpu.HBM)
        dma = pltpu.SemaphoreType.DMA
        return pl.pallas_call(
            functools.partial(moe_kernel, num_ep, local, cap, top_k),
            out_shape=pltpu.VMEM((tok_count, hidden), bf16),
            in_specs=[hbm] * 11,
            out_specs=vm,
            scratch_shapes=[
                pltpu.VMEM((tok_count, hidden), bf16),
                pltpu.VMEM((top_k, tok_count), jnp.int32),
                pltpu.VMEM((top_k, tok_count), jnp.int32),
                pltpu.VMEM((top_k, tok_count), f32),
                pltpu.VMEM((hidden,), bf16),
                pltpu.VMEM((7, tok_count, hidden), bf16),
                pltpu.VMEM((8, 16, tok_count), f32),
                pltpu.VMEM((2, rows, hidden), bf16),
                pltpu.VMEM((rows, hidden), bf16),
                pltpu.VMEM((3, rows, hidden), bf16),
                pltpu.VMEM((SLOTS, hidden, ff), bf16),
                pltpu.VMEM((SLOTS, hidden, ff), bf16),
                pltpu.VMEM((SLOTS, ff, hidden), bf16),
            ] + [pltpu.VMEM((tok_count, hidden), f32)] * 5 + [
                pltpu.VMEM((256, ff), bf16),
                pltpu.VMEM((2 * cap, hidden), bf16),
                pltpu.VMEM((3, CHUNK, 2 * rows), bf16),
                pltpu.VMEM((3, CHUNK, 2 * rows), bf16),
                dma((5,)), dma((SLOTS, 3)), dma((8,)), dma((8,)), dma((7,)), dma((7,)),
                dma, dma((3,)), dma((3, chunks)), dma((3, chunks)),
            ],
            compiler_params=pltpu.CompilerParams(collective_id=0, has_side_effects=True, vmem_limit_bytes=64000000),
        )(expert_ids.T, slots.T, gate_vals.T, tokens, shared_gate, shared_w1, shared_w3, shared_w2, expert_w1, expert_w3, expert_w2)

    return jax.shard_map(device_step, mesh=mesh, in_specs=(row_spec, row_spec, row_spec, row_spec, replicated, replicated, replicated, replicated, expert_spec, expert_spec, expert_spec), out_specs=row_spec, check_vma=False)
```

```python
import functools

import jax
import jax.numpy as jnp
from jax import lax
from jax.experimental import pallas as pl
from jax.experimental.pallas import tpu as pltpu
from jax.sharding import PartitionSpec as P

SLOTS = 3
CHUNK = 128
HEAD = 256
f32, bf16 = jnp.float32, jnp.bfloat16


def dot(a, b):
    return jnp.dot(a, b, preferred_element_type=f32)


def moe_kernel(num_ep, local, cap, top_k, ids_hbm, slot_hbm, gval_hbm, tok_hbm, gate_hbm, sw1, sw3, sw2, ew1, ew3, ew2, out_ref,
               tok_ref, ids_ref, slot_ref, gval_ref, gate_ref, tb, mb, r_mine, r_out, r_in, w1s, w3s, w2s, s1, sd, got1, gotd, got2, h_ref, xs, gma, gmb,
               i_sem, w_sem, t_send, t_recv, m_send, m_recv, r_send, r_recv, s_send, s_recv):
    tok_count, hidden = tok_ref.shape
    ff = w1s.shape[2]
    rows = local * cap
    chunks = tok_count // CHUNK
    me = lax.axis_index('ep')
    core, xx, yy = me % 2, (me // 2) % 2, me // 4
    step_x, step_y = 2 - 4 * xx, 4 - 8 * yy
    part = me + 1 - 2 * core
    n1 = me + (1 - core) * step_x + core * step_y
    n2 = me + core * step_x + (1 - core) * step_y

    def remote(src, dst, ss, rs, dev):
        return pltpu.make_async_remote_copy(src_ref=src, dst_ref=dst, send_sem=ss, recv_sem=rs,
                                            device_id={'ep': dev}, device_id_type=pl.DeviceIdType.MESH)

    def weight_copies(src1, src3, src2, slot):
        return [pltpu.make_async_copy(src1, w1s.at[slot], w_sem.at[slot, 0]),
                pltpu.make_async_copy(src3, w3s.at[slot], w_sem.at[slot, 1]),
                pltpu.make_async_copy(src2, w2s.at[slot], w_sem.at[slot, 2])]

    def start_expert(e, slot):
        for c in weight_copies(ew1.at[e], ew3.at[e], ew2.at[e], slot):
            c.start()

    def start_shared(s, slot):
        cols = pl.ds(s * ff, ff)
        for c in weight_copies(sw1.at[:, cols], sw3.at[:, cols], sw2.at[cols, :], slot):
            c.start()

    def wait_weights(slot):
        for c in weight_copies(ew1.at[0], ew3.at[0], ew2.at[0], slot):
            c.wait()

    barrier = pltpu.get_barrier_semaphore()
    for dev in (n1, n2, part):
        pl.semaphore_signal(barrier, inc=1, device_id={'ep': dev}, device_id_type=pl.DeviceIdType.MESH)
    loads = [pltpu.make_async_copy(src, dst, i_sem.at[k]) for k, (src, dst) in enumerate((
        (ids_hbm, ids_ref), (slot_hbm, slot_ref), (gval_hbm, gval_ref), (tok_hbm, tok_ref), (gate_hbm, gate_ref)))]
    for c in loads:
        c.start()
    loads[3].wait()
    pl.semaphore_wait(barrier, 3)

    class Hop:
        def __init__(self, src, dst, dev):
            self.copies = (remote(mb.at[src], mb.at[dst], m_send.at[dst], m_recv.at[dst], dev),
                           remote(tok_ref if src == 7 else tb.at[src], tb.at[dst], t_send.at[dst], t_recv.at[dst], dev))

        def start(self):
            for c in self.copies:
                c.start()

        def wait_recv(self):
            for c in self.copies:
                c.wait_recv()

        def wait_send(self):
            for c in self.copies:
                c.wait_send()

    t_own, t_n1, t_n1p, t_d, t_dp, t_n2, t_n2p = (
        Hop(7, 0, part), Hop(7, 1, n1), Hop(1, 2, part), Hop(1, 3, n2), Hop(3, 4, part), Hop(7, 5, n2), Hop(5, 6, part))
    head, tail = pl.ds(0, HEAD), pl.ds(HEAD, tok_count - HEAD)
    t_head = remote(tok_ref.at[head], tb.at[5, head], t_send.at[7], t_recv.at[7], n2)
    t_n2.copies = (t_n2.copies[0], remote(tok_ref.at[tail], tb.at[5, tail], t_send.at[5], t_recv.at[5], n2))
    t_n1.copies[1].start()
    t_own.copies[1].start()
    for c in loads[:3] + loads[4:]:
        c.wait()
    for e in range(SLOTS):
        start_expert(e, e)

    kept = slot_ref[...] >= 0
    mb[7, 0:top_k, :] = jnp.where(kept, ids_ref[...] * cap + slot_ref[...], -1).astype(f32)
    mb[7, top_k:2 * top_k, :] = jnp.where(kept, 0.5 * gval_ref[...], 0.0)

    t_n1.copies[0].start()
    t_own.copies[0].start()

    def swiglu_up(x, slot, put):
        full = ff // 256
        for c in range(full):
            cols = slice(c * 256, c * 256 + 256)
            a = dot(x, w1s[slot, :, cols])
            b = dot(x, w3s[slot, :, cols])
            put(cols, (jax.nn.silu(a) * b).astype(bf16))
        cols = slice(full * 256, ff)
        rest = ff - full * 256
        ab = dot(x, jnp.concatenate([w1s[slot, :, cols], w3s[slot, :, cols]], axis=1))
        put(cols, (jax.nn.silu(ab[:, :rest]) * ab[:, rest:]).astype(bf16))

    lane_row = lax.broadcasted_iota(jnp.int32, (cap, tok_count), 0).astype(f32)
    lane_col = lax.broadcasted_iota(jnp.int32, (CHUNK, 128), 1).astype(f32)

    def whole_rows(par):
        return remote(r_out, r_in.at[par], r_send, r_recv.at[par], part)

    def expert_loop(order, par, keep, mine, other, mi, oi, late=()):
        def dispatch(e):
            base = ((me * local + e) * cap).astype(f32)
            for u, (unit, who) in enumerate(((mine, mi), (other, oi))):
                d = mb[who, 0:top_k, :] - base
                hit = d[0:1, :] == lane_row
                for k in range(1, top_k):
                    hit = hit | (d[k:k + 1, :] == lane_row)
                pick = jnp.where(hit, 1.0, 0.0).astype(bf16)
                for n in range(hidden // 256):
                    cols = slice(n * 256, n * 256 + 256)
                    xs[u * cap:(u + 1) * cap, cols] = dot(pick, unit[:, cols]).astype(bf16)

        dispatch(jnp.int32(0))

        def body(e, _):
            for at, what in late:
                pl.when(e == at)(what)
            slot = (order * local + e) % SLOTS
            wait_weights(slot)

            def put(cols, v):
                h_ref[0:2 * cap, cols] = v
            swiglu_up(xs[...], slot, put)
            dispatch(e + 1)
            rs = pl.ds(pl.multiple_of(e * cap, cap), cap)
            for n in range(hidden // 256):
                cols = slice(n * 256, n * 256 + 256)
                v = dot(h_ref[0:2 * cap, :], w2s[slot, :, cols]).astype(bf16)
                r_mine[keep, rs, cols] = v[:cap]
                r_out[rs, cols] = v[cap:]
            remote(r_out.at[rs], r_in.at[par, rs], r_send, r_recv.at[par], part).start()
            if order < 3:
                start_expert((e + SLOTS) % local, slot)
            else:
                @pl.when(e + SLOTS < local)
                def _():
                    start_expert(e + SLOTS, slot)
                for s in range(2):
                    @pl.when(e + SLOTS == local + s)
                    def _():
                        start_shared(s, slot)
            return 0
        lax.fori_loop(0, local, body, 0)

    def combine(par, keep, mi, ready, store, send, wait_rows):
        nr = rows // 128

        def build(i, gm):
            rs = pl.ds(pl.multiple_of(i * CHUNK, CHUNK), CHUNK)
            m = jnp.transpose(mb[mi, :, rs])
            for half, owner in enumerate((me, part)):
                base = (owner * rows).astype(f32)
                for c in range(nr):
                    rid = lane_col + (base + c * 128.0)
                    g = jnp.where(m[:, 0:1] == rid, m[:, top_k:top_k + 1], 0.0)
                    for k in range(1, top_k):
                        g = jnp.where(m[:, k:k + 1] == rid, m[:, top_k + k:top_k + k + 1], g)
                    g1 = g.astype(bf16)
                    rem = g - g1.astype(f32)
                    g2 = rem.astype(bf16)
                    g3 = (rem - g2.astype(f32)).astype(bf16)
                    lanes = slice(half * rows + c * 128, half * rows + c * 128 + 128)
                    gm[0, :, lanes] = g1
                    gm[1, :, lanes] = g2
                    gm[2, :, lanes] = g3

        def products(i, gm):
            rs = pl.ds(pl.multiple_of(i * CHUNK, CHUNK), CHUNK)
            for n in range(hidden // 256):
                cols = slice(n * 256, n * 256 + 256)
                v = None
                for q in range(3):
                    t = dot(gm[q, :, 0:rows], r_mine[keep, :, cols]) + dot(gm[q, :, rows:], r_in[par, :, cols])
                    v = t if v is None else v + t
                store(rs, cols, v + v)

        build(jnp.int32(0), gma)
        wait_rows()

        def pair(j, _):
            for t, (now, later) in enumerate(((gma, gmb), (gmb, gma))):
                i = 2 * j + t
                rs = pl.ds(pl.multiple_of(i * CHUNK, CHUNK), CHUNK)
                ready(i, rs)
                build((i + 1) % chunks, later)
                products(i, now)
                send(i, rs)
            return 0
        lax.fori_loop(0, chunks // 2, pair, 0)

    def chunk_rows(c):
        return pl.ds(c * CHUNK, CHUNK)

    def s_copy(which, c, rs):
        src, dst, dev = ((s1, got1, n1), (sd, gotd, n1), (s1, got2, n2))[which]
        return remote(src.at[rs], dst.at[rs], s_send.at[which, c], s_recv.at[which, c], dev)

    def put_s1(rs, cols, v):
        s1[rs, cols] = v

    def put_sd(rs, cols, v):
        sd[rs, cols] = v

    def put_s2(rs, cols, v):
        s1[rs, cols] = v + gotd[rs, cols]

    def nothing(i, rs):
        pass

    def first_tokens():
        t_n1.wait_recv()
        t_d.start()
        t_n1p.start()
        t_n2.start()

    t_own.wait_recv()
    expert_loop(0, 2, 1, tok_ref, tb.at[0], 7, 0, late=((local - 3, t_head.start), (local - 1, first_tokens)))
    t_n1p.wait_recv()
    whole_rows(2).wait_send()

    expert_loop(1, 0, 0, tb.at[1], tb.at[2], 1, 2)
    t_d.wait_recv()
    t_dp.start()
    combine(0, 0, 1, nothing, put_s1, lambda i, rs: s_copy(0, i, rs).start(), lambda: whole_rows(0).wait())
    t_dp.wait_recv()

    expert_loop(2, 1, 0, tb.at[3], tb.at[4], 3, 4)
    t_head.wait_recv()
    t_n2.wait_recv()
    t_n2p.start()
    combine(1, 0, 3, nothing, put_sd, lambda i, rs: s_copy(1, i, rs).start(), lambda: whole_rows(1).wait())
    t_n2p.wait_recv()

    expert_loop(3, 0, 0, tb.at[5], tb.at[6], 5, 6)
    for c in range(chunks):
        s_copy(0, c, chunk_rows(c)).wait_send()
    combine(0, 0, 5, lambda i, rs: s_copy(1, i, rs).wait_recv(), put_s2, lambda i, rs: s_copy(2, i, rs).start(),
            lambda: whole_rows(0).wait())

    for c in range(chunks):
        s_copy(1, c, chunk_rows(c)).wait_send()
    combine(2, 1, 7, nothing, put_sd, nothing, lambda: whole_rows(2).wait_recv())

    mrows = 256
    for c in range(chunks):
        s_copy(0, c, chunk_rows(c)).wait_recv()
    for s in range(2):
        slot = (4 * local + s) % SLOTS
        wait_weights(slot)

        def block(i, _):
            rs = pl.ds(pl.multiple_of(i * mrows, mrows), mrows)

            def put(cols, v):
                h_ref[:, cols] = v
            swiglu_up(tok_ref[rs, :], slot, put)
            logit = jnp.sum(tok_ref[rs, :].astype(f32) * gate_ref[...].astype(f32).reshape(1, hidden), axis=1, keepdims=True)
            sig = jax.nn.sigmoid(logit)
            for n in range(hidden // 256):
                cols = slice(n * 256, n * 256 + 256)
                v = sd[rs, cols] + sig * dot(h_ref[...], w2s[slot, :, cols])
                if s == 1:
                    v = v + tok_ref[rs, cols].astype(f32) + got1[rs, cols]
                sd[rs, cols] = v
            return 0
        lax.fori_loop(0, tok_count // mrows, block, 0)

    for c in range(chunks):
        rs = chunk_rows(c)
        s_copy(2, c, rs).wait_recv()
        out_ref[rs, :] = (sd[rs, :] + got2[rs, :]).astype(bf16)
    for c in range(chunks):
        rs = chunk_rows(c)
        s_copy(2, c, rs).wait_send()
    for t in (t_head, t_own, t_n1, t_n1p, t_d, t_dp, t_n2, t_n2p):
        t.wait_send()


def solution(mesh):
    num_ep = mesh.shape['ep']
    row_spec = P(('dp', 'ep'), None)
    replicated = P()
    expert_spec = P('ep', None, None)

    def device_step(tokens, expert_ids, gate_vals, slots, shared_w1, shared_w3, shared_w2, shared_gate, expert_w1, expert_w3, expert_w2):
        tok_count, hidden = tokens.shape
        top_k = expert_ids.shape[1]
        local, _, ff = expert_w1.shape
        num_experts = local * num_ep
        cap = 8 * ((2 * tok_count * top_k + 8 * num_experts - 1) // (8 * num_experts))
        rows = local * cap
        chunks = tok_count // CHUNK
        vm = pl.BlockSpec(memory_space=pltpu.VMEM)
        hbm = pl.BlockSpec(memory_space=pltpu.HBM)
        dma = pltpu.SemaphoreType.DMA
        return pl.pallas_call(
            functools.partial(moe_kernel, num_ep, local, cap, top_k),
            out_shape=pltpu.VMEM((tok_count, hidden), bf16),
            in_specs=[hbm] * 11,
            out_specs=vm,
            scratch_shapes=[
                pltpu.VMEM((tok_count, hidden), bf16),
                pltpu.VMEM((top_k, tok_count), jnp.int32),
                pltpu.VMEM((top_k, tok_count), jnp.int32),
                pltpu.VMEM((top_k, tok_count), f32),
                pltpu.VMEM((hidden,), bf16),
                pltpu.VMEM((7, tok_count, hidden), bf16),
                pltpu.VMEM((8, 2 * top_k, tok_count), f32),
                pltpu.VMEM((2, rows, hidden), bf16),
                pltpu.VMEM((rows, hidden), bf16),
                pltpu.VMEM((3, rows, hidden), bf16),
                pltpu.VMEM((SLOTS, hidden, ff), bf16),
                pltpu.VMEM((SLOTS, hidden, ff), bf16),
                pltpu.VMEM((SLOTS, ff, hidden), bf16),
            ] + [pltpu.VMEM((tok_count, hidden), f32)] * 5 + [
                pltpu.VMEM((256, ff), bf16),
                pltpu.VMEM((2 * cap, hidden), bf16),
                pltpu.VMEM((3, CHUNK, 2 * rows), bf16),
                pltpu.VMEM((3, CHUNK, 2 * rows), bf16),
                dma((5,)), dma((SLOTS, 3)), dma((8,)), dma((8,)), dma((7,)), dma((7,)),
                dma, dma((3,)), dma((3, chunks)), dma((3, chunks)),
            ],
            compiler_params=pltpu.CompilerParams(collective_id=0, has_side_effects=True, vmem_limit_bytes=64000000),
        )(expert_ids.T, slots.T, gate_vals.T, tokens, shared_gate, shared_w1, shared_w3, shared_w2, expert_w1, expert_w3, expert_w2)

    return jax.shard_map(device_step, mesh=mesh, in_specs=(row_spec, row_spec, row_spec, row_spec, replicated, replicated, replicated, replicated, expert_spec, expert_spec, expert_spec), out_specs=row_spec, check_vma=False)
```
